32 devices in a mesh: dp: 1 (over z), ei: 4 (over y), eo: 8 (over x, core).
Axes of the slice: x: 4, y: 4, z: 1, core: 2. Of those that a mesh axis runs over, the one named last changes fastest.
The devices are a block of a 4x4x8 slice.
Arguments:
- x_in: bfloat16 [8192, 1024], P(('dp', 'ei', 'eo'))
- expert_idx: int32 [8192, 8], P(('dp', 'ei', 'eo'))
- gate_val: float32 [8192, 8], P(('dp', 'ei', 'eo'))
- w_gate: bfloat16 [32, 1024, 512], P(('ei', 'eo'))
- w_up: bfloat16 [32, 1024, 512], P(('ei', 'eo'))
- w_down: bfloat16 [32, 512, 1024], P(('ei', 'eo'))
- dy_in: bfloat16 [8192, 1024], P(('dp', 'ei', 'eo'))
Outputs:
- output 1: bfloat16 [8192, 1024], P(('dp', 'ei', 'eo'))
- output 2: bfloat16 [8192, 1024], P(('dp', 'ei', 'eo'))
- output 3: float32 [8192, 8], P(('dp', 'ei', 'eo'))
- output 4: float32 [32, 1024, 512], P(('dp', 'ei', 'eo'))
- output 5: float32 [32, 1024, 512], P(('dp', 'ei', 'eo'))
- output 6: float32 [32, 512, 1024], P(('dp', 'ei', 'eo'))
All inputs are finite; a program needn't handle non-finite values.
Results may differ from the reference program's by a relative error of at most 0.00784527.
Values are sent between devices in bfloat16 or wider.
A program may use at most 768 MiB of HBM per device.

```python
import jax
import jax.numpy as jnp
from jax import lax

TOKENS_DEV = 256
GROUP_DEVS = 32
D_MODEL = 1024
FF_EXPERT = 512
EXPERTS = 32
TOP_K = 8
SKEW_FACTOR = 4

CAPACITY = SKEW_FACTOR * ((TOKENS_DEV * TOP_K + EXPERTS - 1) // EXPERTS)
ROWS_EXPERT = GROUP_DEVS * CAPACITY
HOT_EXPERTS = EXPERTS // 8
REST_LOAD = TOKENS_DEV * TOP_K - HOT_EXPERTS * CAPACITY
REST_BASE = REST_LOAD // (EXPERTS - HOT_EXPERTS)
REST_EXTRA = REST_LOAD % (EXPERTS - HOT_EXPERTS)


def draw_routing(dev_key):
    perm_key, tok_key, col_key = jax.random.split(dev_key, 3)
    rank_ids = jnp.arange(EXPERTS, dtype=jnp.int32)
    extra_one = ((rank_ids - HOT_EXPERTS) < REST_EXTRA).astype(jnp.int32)
    load_by_rank = jnp.where(rank_ids < HOT_EXPERTS, CAPACITY, REST_BASE + extra_one).astype(jnp.int32)
    expert_perm = jax.random.permutation(perm_key, EXPERTS)
    exp_loads = jnp.zeros((EXPERTS,), jnp.int32).at[expert_perm].set(load_by_rank)
    load_ends = jnp.cumsum(exp_loads)
    positions = jnp.arange(TOKENS_DEV * TOP_K, dtype=jnp.int32)
    expert_list = jnp.searchsorted(load_ends, positions, side='right').astype(jnp.int32)
    base_idx = expert_list.reshape(TOP_K, TOKENS_DEV).T
    tok_perm = jax.random.permutation(tok_key, TOKENS_DEV)
    col_score = jax.random.randint(col_key, (TOKENS_DEV, TOP_K), 0, 1 << 20) * TOP_K + jnp.arange(TOP_K, dtype=jnp.int32)
    col_perm = jnp.argsort(col_score, axis=1)
    return jnp.take_along_axis(base_idx[tok_perm], col_perm, axis=1).astype(jnp.int32)


def setup_inputs(seed: int = 0, part: int = 0) -> dict:
    root_key = jax.random.key(seed)
    part_root, shared_root = jax.random.split(root_key)
    part_key = jax.random.fold_in(part_root, part)
    x_key, route_key, gate_key, dy_key = jax.random.split(part_key, 4)
    wg_key, wu_key, wd_key = jax.random.split(shared_root, 3)
    n_tok = GROUP_DEVS * TOKENS_DEV
    dev_keys = jax.random.split(route_key, GROUP_DEVS)
    expert_idx = jax.vmap(draw_routing)(dev_keys).reshape(n_tok, TOP_K)
    x_in = jax.random.normal(x_key, (n_tok, D_MODEL), jnp.float32).astype(jnp.bfloat16)
    gate_val = jax.random.uniform(gate_key, (n_tok, TOP_K), jnp.float32, 0.05, 0.3)
    w_gate = (jax.random.normal(wg_key, (EXPERTS, D_MODEL, FF_EXPERT), jnp.float32) * D_MODEL ** -0.5).astype(jnp.bfloat16)
    w_up = (jax.random.normal(wu_key, (EXPERTS, D_MODEL, FF_EXPERT), jnp.float32) * D_MODEL ** -0.5).astype(jnp.bfloat16)
    w_down = (jax.random.normal(wd_key, (EXPERTS, FF_EXPERT, D_MODEL), jnp.float32) * FF_EXPERT ** -0.5).astype(jnp.bfloat16)
    dy_in = jax.random.normal(dy_key, (n_tok, D_MODEL), jnp.float32).astype(jnp.bfloat16)
    return {'x_in': x_in, 'expert_idx': expert_idx, 'gate_val': gate_val, 'w_gate': w_gate, 'w_up': w_up, 'w_down': w_down, 'dy_in': dy_in}


def expert_pass(x_rows, do_rows, w_gate_e, w_up_e, w_down_e):
    pre_gate = jnp.dot(x_rows, w_gate_e, preferred_element_type=jnp.float32)
    pre_up = jnp.dot(x_rows, w_up_e, preferred_element_type=jnp.float32)
    sig_gate = jax.nn.sigmoid(pre_gate)
    silu_gate = pre_gate * sig_gate
    hidden = (silu_gate * pre_up).astype(jnp.bfloat16)
    out_rows = jnp.dot(hidden, w_down_e, preferred_element_type=jnp.float32).astype(jnp.bfloat16)
    dw_down_e = jnp.dot(hidden.T, do_rows, preferred_element_type=jnp.float32)
    d_hidden = jnp.dot(do_rows, w_down_e.T, preferred_element_type=jnp.float32)
    d_gate = (d_hidden * pre_up * sig_gate * (1.0 + pre_gate * (1.0 - sig_gate))).astype(jnp.bfloat16)
    d_up = (d_hidden * silu_gate).astype(jnp.bfloat16)
    dw_gate_e = jnp.dot(x_rows.T, d_gate, preferred_element_type=jnp.float32)
    dw_up_e = jnp.dot(x_rows.T, d_up, preferred_element_type=jnp.float32)
    dx_rows = (jnp.dot(d_gate, w_gate_e.T, preferred_element_type=jnp.float32) + jnp.dot(d_up, w_up_e.T, preferred_element_type=jnp.float32)).astype(jnp.bfloat16)
    return out_rows, dx_rows, dw_gate_e, dw_up_e, dw_down_e


def reference(x_in, expert_idx, gate_val, w_gate, w_up, w_down, dy_in):
    n_tok = GROUP_DEVS * TOKENS_DEV
    n_assign = n_tok * TOP_K
    flat_exp = expert_idx.reshape(n_assign)
    sort_order = jnp.argsort(flat_exp, stable=True).astype(jnp.int32)
    sorted_exp = flat_exp[sort_order]
    counts = jax.ops.segment_sum(jnp.ones((n_assign,), jnp.int32), flat_exp, num_segments=EXPERTS)
    starts = jnp.cumsum(counts) - counts
    within = jnp.arange(n_assign, dtype=jnp.int32) - starts[sorted_exp]
    slot_sorted = (sorted_exp * ROWS_EXPERT + within).astype(jnp.int32)
    slot_of = jnp.zeros((n_assign,), jnp.int32).at[sort_order].set(slot_sorted)
    slot_owner = jnp.full((EXPERTS * ROWS_EXPERT,), -1, jnp.int32).at[slot_sorted].set(sort_order)
    has_row = slot_owner >= 0
    safe_owner = jnp.where(has_row, slot_owner, 0)
    tok_of_slot = safe_owner // TOP_K
    slot_gate = jnp.where(has_row, gate_val.reshape(n_assign)[safe_owner], 0.0)

    def one_expert(operands):
        tok_ids, gate_rows, w_gate_e, w_up_e, w_down_e = operands
        x_rows = x_in[tok_ids]
        do_rows = (gate_rows[:, None] * dy_in[tok_ids]).astype(jnp.bfloat16)
        return expert_pass(x_rows, do_rows, w_gate_e, w_up_e, w_down_e)

    out_rows, dx_rows, dw_gate, dw_up, dw_down = lax.map(one_expert, (tok_of_slot.reshape(EXPERTS, ROWS_EXPERT), slot_gate.reshape(EXPERTS, ROWS_EXPERT), w_gate, w_up, w_down))
    out_tok = out_rows.reshape(EXPERTS * ROWS_EXPERT, D_MODEL)[slot_of].reshape(n_tok, TOP_K, D_MODEL).astype(jnp.float32)
    y_out = jnp.sum(gate_val[:, :, None] * out_tok, axis=1).astype(jnp.bfloat16)
    dgate_out = jnp.sum(dy_in.astype(jnp.float32)[:, None, :] * out_tok, axis=2)
    dx_tok = dx_rows.reshape(EXPERTS * ROWS_EXPERT, D_MODEL)[slot_of].reshape(n_tok, TOP_K, D_MODEL).astype(jnp.float32)
    dx_out = jnp.sum(dx_tok, axis=1).astype(jnp.bfloat16)
    return (y_out, dx_out, dgate_out, dw_gate, dw_up, dw_down)
```

```python
import jax
import jax.numpy as jnp
from jax import lax
from jax.sharding import PartitionSpec as P

GROUP = ('ei', 'eo')


def solution(mesh):
    ei_size = mesh.shape['ei']
    eo_size = mesh.shape['eo']
    group_devs = ei_size * eo_size
    tok_spec = P(('dp', 'ei', 'eo'), None)
    weight_spec = P(('ei', 'eo'), None, None)
    grad_spec = P(('dp', 'ei', 'eo'), None, None)

    def dot(a, b, dims):
        return lax.dot_general(a, b, (dims, ((), ())), preferred_element_type=jnp.float32)

    def device_layer(x_loc, idx_loc, gate_loc, wg_loc, wu_loc, wd_loc, dy_loc):
        tok_count, top_k = idx_loc.shape
        wg, wu, wd = wg_loc[0], wu_loc[0], wd_loc[0]
        me = lax.axis_index(GROUP)
        hit = idx_loc[None, :, :] == jnp.arange(group_devs, dtype=jnp.int32)[:, None, None]
        gate_dense = jnp.sum(jnp.where(hit, gate_loc[None], 0.0), axis=2)
        gates = lax.all_to_all(gate_dense, GROUP, 0, 0, tiled=True)
        gates = gates.reshape(group_devs * tok_count, 1)
        x_all = lax.all_gather(x_loc, GROUP, axis=0, tiled=True)
        dy_all = lax.all_gather(dy_loc, GROUP, axis=0, tiled=True)
        a = dot(x_all, wg, ((1,), (0,)))
        b = dot(x_all, wu, ((1,), (0,)))
        s = jax.nn.sigmoid(a)
        h = (a * s * b).astype(jnp.bfloat16)
        o = dot(h, wd, ((1,), (0,))).astype(jnp.bfloat16)
        y_part = gates * o
        y_loc = lax.psum_scatter(y_part, GROUP, scatter_dimension=0, tiled=True).astype(jnp.bfloat16)
        dg = jnp.sum(dy_all.astype(jnp.float32) * o.astype(jnp.float32), axis=1)
        dg = lax.all_to_all(dg.reshape(group_devs, tok_count), GROUP, 0, 0, tiled=True)
        dgate_loc = jnp.sum(jnp.where(hit, dg[:, :, None], 0.0), axis=0)
        g = (gates * dy_all).astype(jnp.bfloat16)
        dw_down = dot(h, g, ((0,), (0,)))
        dh = dot(g, wd, ((1,), (1,)))
        da = (dh * b * s * (1.0 + a * (1.0 - s))).astype(jnp.bfloat16)
        db = (dh * (a * s)).astype(jnp.bfloat16)
        dx_rows = (dot(da, wg, ((1,), (1,))) + dot(db, wu, ((1,), (1,)))).astype(jnp.bfloat16)
        dx_loc = lax.psum_scatter(dx_rows.astype(jnp.float32), GROUP, scatter_dimension=0, tiled=True).astype(jnp.bfloat16)
        dw_gate = dot(x_all, da, ((0,), (0,)))
        dw_up = dot(x_all, db, ((0,), (0,)))
        return y_loc, dx_loc, dgate_loc, dw_gate[None], dw_up[None], dw_down[None]

    return jax.shard_map(device_layer, mesh=mesh, in_specs=(tok_spec, tok_spec, tok_spec, weight_spec, weight_spec, weight_spec, tok_spec), out_specs=(tok_spec, tok_spec, tok_spec, grad_spec, grad_spec, grad_spec), check_vma=False)
```

```python
import functools

import jax
import jax.numpy as jnp
from jax import lax
from jax.experimental import pallas as pl
from jax.experimental.pallas import tpu as pltpu
from jax.sharding import PartitionSpec as P

MESH = pl.DeviceIdType.MESH
RINGS = 4
CORES = 2
SLOTS = 4
LANES = 128
F32 = jnp.float32
BF16 = jnp.bfloat16


def dot(a, b, dim_a, dim_b):
    return lax.dot_general(a, b, (((dim_a,), (dim_b,)), ((), ())), preferred_element_type=F32)


def kernel(nx, ny, x_hbm, dy_hbm, gt_hbm, wg_hbm, wu_hbm, wd_hbm,
           y_out, dx_out, dgt_out, dwg_out, dwu_out, dwd_out,
           xy, gt, acc, accg, con, cong, wg, wu, wd, dwg, dwu, dwd, rwg, rwu, rwd,
           loc_sem, xs, xr, gs, gr, acs, acr, ags, agr, ws, wr, ds, dr, free_x, free_a):
    steps = nx * ny
    dp = lax.axis_index('dp')
    row = lax.axis_index('ei')
    eo = lax.axis_index('eo')
    col, core = eo // CORES, eo % CORES
    experts = steps * CORES
    expert_ids = (row * nx * CORES + eo, row * nx * CORES + col * CORES + (1 - core))

    def dev(c, r):
        return (dp, (r + ny) % ny, ((c + nx) % nx) * CORES + core)

    turn = ((col + row) % nx) // (nx - 1)
    back = ((col + row + nx - 1) % nx) // (nx - 1)
    up_a, dn_a = dev(col + 1 - turn, row + turn), dev(col - 1 + back, row - back)
    up_b, dn_b = dev(col + turn, row + 1 - turn), dev(col - back, row - 1 + back)
    nxt = (up_a, dn_a, up_b, dn_b)
    prv = (dn_a, up_a, dn_b, up_b)
    mate = (dp, row, col * CORES + (1 - core))

    loads = [pltpu.make_async_copy(s, d, loc_sem.at[i]) for i, (s, d) in enumerate((
        (x_hbm, xy.at[0, 0]), (dy_hbm, xy.at[0, 1]), (gt_hbm, gt.at[0]),
        (wg_hbm, wg.at[0]), (wu_hbm, wu.at[0]), (wd_hbm, wd.at[0])))]
    for load in loads:
        load.start()

    barrier = pltpu.get_barrier_semaphore()
    for peer in nxt + (mate,):
        pl.semaphore_signal(barrier, inc=1, device_id=peer, device_id_type=MESH)
    pl.semaphore_wait(barrier, RINGS + 1)

    def remote(src, dst, send, recv, peer):
        return pltpu.make_async_remote_copy(src_ref=src, dst_ref=dst, send_sem=send, recv_sem=recv, device_id=peer, device_id_type=MESH)

    weights = [remote(s, d.at[1], ws.at[i], wr.at[i], mate) for i, (s, d) in enumerate(((wg_hbm, wg), (wu_hbm, wu), (wd_hbm, wd)))]
    grads = [remote(s.at[1], d, ds.at[i], dr.at[i], mate) for i, (s, d) in enumerate(((dwg, rwg), (dwu, rwu), (dwd, rwd)))]

    def fwd(s, r):
        a, b = s % SLOTS, (s + 1) % SLOTS
        return (remote(xy.at[a, :, r], xy.at[b, :, r], xs.at[a, r], xr.at[b, r], nxt[r]),
                remote(gt.at[a, r], gt.at[b, r], gs.at[a, r], gr.at[b, r], nxt[r]))

    def push(s, k, r):
        a, b = s % SLOTS, (s + 1) % SLOTS
        return remote(acc.at[a, k, r], acc.at[b, k, r], acs.at[a, k, r], acr.at[b, k, r], nxt[r])

    def pushg(s, r):
        a, b = s % SLOTS, (s + 1) % SLOTS
        return remote(accg.at[a, r], accg.at[b, r], ags.at[a, r], agr.at[b, r], nxt[r])

    for load in loads[:3]:
        load.wait()
    for r in range(RINGS):
        for c in fwd(0, r):
            c.start()
    for w in weights:
        w.start()
    for ref in (dwg, dwu, dwd):
        ref[...] = jnp.zeros_like(ref)
    for load in loads[3:]:
        load.wait()

    tr = xy.shape[3]
    d_model = xy.shape[4]
    tok = RINGS * tr
    groups = LANES // experts
    pk = tr // groups
    lane = lax.broadcasted_iota(jnp.int32, (pk, LANES), 1)

    def compute(s):
        slot = s % SLOTS
        which = jnp.minimum(s, 1)
        for e in range(CORES):
            if e == 1:
                @pl.when(s == 0)
                def _():
                    for w in weights:
                        w.wait()
            gate = jnp.concatenate([
                jnp.sum(jnp.where(lane == q * experts + expert_ids[e], gt[slot, r], 0.0), axis=1, keepdims=True)
                for r in range(RINGS) for q in range(groups)], axis=0)
            x = xy[slot, 0].reshape(tok, d_model)
            dy = xy[slot, 1].reshape(tok, d_model)
            xm = x * jnp.where(gate > 0.0, 1.0, 0.0).astype(BF16)
            a = dot(xm, wg[e], 1, 0)
            b = dot(xm, wu[e], 1, 0)
            sig = jax.nn.sigmoid(a)
            silu = a * sig
            h = (silu * b).astype(BF16)
            o = dot(h, wd[e], 1, 0).astype(BF16).astype(F32)
            dy32 = dy.astype(F32)
            dg = jnp.sum(dy32 * o, axis=1, keepdims=True)
            g32 = gate * dy32
            g = g32.astype(BF16)
            yc = (gate * o).reshape(RINGS, tr, d_model)
            packed = [functools.reduce(lambda p, v: p + v, [
                jnp.where(lane == q * experts + expert_ids[e], dg[(r * groups + q) * pk:(r * groups + q + 1) * pk], 0.0)
                for q in range(groups)]) for r in range(RINGS)]
            if e == 0:
                con[which, 0] = yc
                for r in range(RINGS):
                    cong[which, r] = packed[r]
            else:
                con[which, 0] += yc
                for r in range(RINGS):
                    cong[which, r] += packed[r]
            dwd[e] += dot(h, g, 0, 0)
            dh = dot(g, wd[e], 1, 1)
            da = (dh * b * sig * (1.0 + a * (1.0 - sig))).astype(BF16)
            db = (dh * silu).astype(BF16)
            dxc = (dot(da, wg[e], 1, 1) + dot(db, wu[e], 1, 1)).astype(BF16).astype(F32).reshape(RINGS, tr, d_model)
            if e == 0:
                con[which, 1] = dxc
            else:
                con[which, 1] += dxc
            dwg[e] += dot(x, da, 0, 0)
            dwu[e] += dot(x, db, 0, 0)

    def step(s, _):
        slot = s % SLOTS
        compute(s)

        @pl.when(s < steps - 1)
        def _():
            for r in range(RINGS):
                for c in fwd(s, r):
                    c.wait_recv()

        @pl.when(s < steps - 2)
        def _():
            for r in range(RINGS):
                @pl.when(s + 2 >= SLOTS)
                def _():
                    pl.semaphore_wait(free_x.at[r], 1)
                for c in fwd(s + 1, r):
                    c.start()

        @pl.when(s == steps - 1)
        def _():
            for c in grads:
                c.start()

        @pl.when(s >= 1)
        def _():
            for k in range(2):
                for r in range(RINGS):
                    @pl.when(s == 1)
                    def _():
                        acc[slot, k, r] = con[1, k, r]

                    @pl.when(s >= 2)
                    def _():
                        push(s - 1, k, r).wait_recv()
                        acc[slot, k, r] += con[1, k, r]
                    if k == 0:
                        @pl.when(s == 1)
                        def _():
                            accg[slot, r] = cong[1, r]

                        @pl.when(s >= 2)
                        def _():
                            pushg(s - 1, r).wait_recv()
                            accg[slot, r] += cong[1, r]
                for r in range(RINGS):
                    if k == 0:
                        @pl.when(s >= SLOTS)
                        def _():
                            pl.semaphore_wait(free_a.at[r], 1)
                    push(s, k, r).start()
                    if k == 1:
                        pushg(s, r).start()

        @pl.when((s >= 1) & (s <= steps - 1))
        def _():
            for r in range(RINGS):
                for c in fwd(s - 1, r):
                    c.wait_send()

                @pl.when(s <= steps - SLOTS)
                def _():
                    pl.semaphore_signal(free_x.at[r], inc=1, device_id=prv[r], device_id_type=MESH)

        @pl.when(s >= 2)
        def _():
            for r in range(RINGS):
                for k in range(2):
                    push(s - 1, k, r).wait_send()
                pushg(s - 1, r).wait_send()

                @pl.when(s - 1 <= steps - SLOTS)
                def _():
                    pl.semaphore_signal(free_a.at[r], inc=1, device_id=prv[r], device_id_type=MESH)
        return 0

    lax.fori_loop(0, steps, step, 0)

    home = steps % SLOTS
    for c in grads:
        c.wait()
    dwg_out[...] = dwg[0] + rwg[...]
    dwu_out[...] = dwu[0] + rwu[...]
    dwd_out[...] = dwd[0] + rwd[...]
    for r in range(RINGS):
        rows = pl.ds(r * tr, tr)
        for k, out in ((0, y_out), (1, dx_out)):
            push(steps - 1, k, r).wait()
            out[rows, :] = (acc[home, k, r] + con[0, k, r]).astype(BF16)
        pushg(steps - 1, r).wait()
        dgt_out[r] = accg[home, r] + cong[0, r]


def solution(mesh):
    ny = mesh.shape['ei']
    nx = mesh.shape['eo'] // CORES
    experts = ny * nx * CORES
    groups = LANES // experts
    tok_spec = P(('dp', 'ei', 'eo'), None)
    weight_spec = P(('ei', 'eo'), None, None)
    grad_spec = P(('dp', 'ei', 'eo'), None, None)
    hbm = pl.BlockSpec(memory_space=pl.ANY)
    vmem = pl.BlockSpec(memory_space=pltpu.VMEM)

    def device_layer(x_loc, idx_loc, gate_loc, wg_loc, wu_loc, wd_loc, dy_loc):
        tok, _ = idx_loc.shape
        d_model = x_loc.shape[1]
        d_ff = wg_loc.shape[2]
        tr = tok // RINGS
        pk = tr // groups
        hit = idx_loc[:, :, None] == jnp.arange(experts, dtype=jnp.int32)
        gates = jnp.sum(jnp.where(hit, gate_loc[:, :, None], 0.0), axis=1)
        gates = gates.reshape(RINGS, groups, pk, experts).transpose(0, 2, 1, 3).reshape(RINGS, pk, LANES)
        dma = pltpu.SemaphoreType.DMA
        steps = nx * ny
        row_bytes = tok * d_model
        y_loc, dx_loc, dgt, dwg, dwu, dwd = pl.pallas_call(
            functools.partial(kernel, nx, ny),
            out_shape=(
                jax.ShapeDtypeStruct((tok, d_model), BF16), jax.ShapeDtypeStruct((tok, d_model), BF16),
                jax.ShapeDtypeStruct((RINGS, pk, LANES), F32),
                jax.ShapeDtypeStruct((d_model, d_ff), F32), jax.ShapeDtypeStruct((d_model, d_ff), F32),
                jax.ShapeDtypeStruct((d_ff, d_model), F32)),
            in_specs=[hbm] * 6,
            out_specs=(vmem,) * 6,
            scratch_shapes=[
                pltpu.VMEM((SLOTS, 2, RINGS, tr, d_model), BF16),
                pltpu.VMEM((SLOTS, RINGS, pk, LANES), F32),
                pltpu.VMEM((SLOTS, 2, RINGS, tr, d_model), F32),
                pltpu.VMEM((SLOTS, RINGS, pk, LANES), F32),
                pltpu.VMEM((2, 2, RINGS, tr, d_model), F32),
                pltpu.VMEM((2, RINGS, pk, LANES), F32),
                pltpu.VMEM((CORES, d_model, d_ff), BF16), pltpu.VMEM((CORES, d_model, d_ff), BF16), pltpu.VMEM((CORES, d_ff, d_model), BF16),
                pltpu.VMEM((CORES, d_model, d_ff), F32), pltpu.VMEM((CORES, d_model, d_ff), F32), pltpu.VMEM((CORES, d_ff, d_model), F32),
                pltpu.VMEM((d_model, d_ff), F32), pltpu.VMEM((d_model, d_ff), F32), pltpu.VMEM((d_ff, d_model), F32),
                dma((6,)), dma((SLOTS, RINGS)), dma((SLOTS, RINGS)), dma((SLOTS, RINGS)), dma((SLOTS, RINGS)),
                dma((SLOTS, 2, RINGS)), dma((SLOTS, 2, RINGS)), dma((SLOTS, RINGS)), dma((SLOTS, RINGS)),
                dma((3,)), dma((3,)), dma((3,)), dma((3,)),
                pltpu.SemaphoreType.REGULAR((RINGS,)), pltpu.SemaphoreType.REGULAR((RINGS,)),
            ],
            compiler_params=pltpu.CompilerParams(collective_id=0, has_side_effects=True, vmem_limit_bytes=66000000),
            cost_estimate=pl.CostEstimate(flops=18 * steps * row_bytes * d_ff * CORES, bytes_accessed=steps * row_bytes * 12, transcendentals=0),
        )(x_loc.reshape(RINGS, tr, d_model), dy_loc.reshape(RINGS, tr, d_model), gates, wg_loc[0], wu_loc[0], wd_loc[0])
        dgt = dgt.reshape(RINGS, pk, groups, experts).transpose(0, 2, 1, 3).reshape(tok, experts)
        dgate_loc = jnp.sum(jnp.where(hit, dgt[:, None, :], 0.0), axis=2)
        return y_loc, dx_loc, dgate_loc, dwg[None], dwu[None], dwd[None]

    return jax.shard_map(device_layer, mesh=mesh, in_specs=(tok_spec, tok_spec, tok_spec, weight_spec, weight_spec, weight_spec, tok_spec), out_specs=(tok_spec, tok_spec, tok_spec, grad_spec, grad_spec, grad_spec), check_vma=False)
```

```python
import functools

import jax
import jax.numpy as jnp
from jax import lax
from jax.experimental import pallas as pl
from jax.experimental.pallas import tpu as pltpu
from jax.sharding import PartitionSpec as P

MESH = pl.DeviceIdType.MESH
SIDE = 4
CORES = 2
LANES = 128
F32 = jnp.float32
BF16 = jnp.bfloat16
N_MSG = 96


def dot(a, b, dim_a, dim_b):
    return lax.dot_general(a, b, (((dim_a,), (dim_b,)), ((), ())), preferred_element_type=F32)


def kernel(x_hbm, dy_hbm, gt_hbm, wg_hbm, wu_hbm, wd_hbm,
           y_out, dx_out, dgt_out, dwg_out, dwu_out, dwd_out, whg, whu, whd,
           xyc, xyo, gtc, gto, con, cong, rsh, rshg, rsf, rsfg, wg, wu, wd, dwg, dwu, dwd,
           send_sem, recv_sem, loc_sem, wl_sem):
    dp = lax.axis_index('dp')
    row = lax.axis_index('ei')
    eo = lax.axis_index('eo')
    col, core = eo // CORES, eo % CORES
    experts = SIDE * SIDE * CORES

    def dev(c, r, k):
        return (dp, (r + SIDE) % SIDE, ((c + SIDE) % SIDE) * CORES + k)

    xpeer = (dev(col + 1, row, core), dev(col - 1, row, core))
    ypeer = (dev(col, row + 1, core), dev(col, row - 1, core))
    mate = dev(col, row, 1 - core)

    def expert_id(p, i):
        return row * SIDE * CORES + ((col + i) % SIDE) * CORES + (core + p) % CORES

    msgs = {}

    def msg(name, src, dst, peer):
        n = len(msgs)
        assert n < N_MSG
        msgs[name] = pltpu.make_async_remote_copy(
            src_ref=src, dst_ref=dst, send_sem=send_sem.at[n], recv_sem=recv_sem.at[n], device_id=peer, device_id_type=MESH)

    d_ff2, d_model2 = wd.shape[1] // 2, wg.shape[1] // 2
    wins, whs, halves = (wg_hbm, wu_hbm, wd_hbm), (whg, whu, whd), (d_model2, d_model2, d_ff2)
    for d in range(2):
        at, frm = (3, 1)[d], (3, 1)[d]
        msg(('x1', d), xyc.at[0, :, 0], xyo.at[at - 1, 0, :, 0], xpeer[d])
        msg(('x1g', d), gtc.at[0, 0], gto.at[at - 1, 0, 0], xpeer[d])
        k = 1 - d
        msg(('x2', d), xyo.at[frm - 1, 0, k, 0], xyo.at[1, 0, k, 0], xpeer[d])
        for m in range(3):
            msg(('w1', m, d), wins[m], whs[m].at[0, at], xpeer[d])
            rows = pl.ds(d * halves[m], halves[m])
            msg(('w2', m, d), whs[m].at[0, frm, rows], whs[m].at[0, 2, rows], xpeer[d])
        msg(('y1', d), xyc.at[0], xyc.at[at], ypeer[d])
        msg(('y1g', d), gtc.at[0], gtc.at[at], ypeer[d])
        msg(('y2', d), xyc.at[frm, :, d], xyc.at[2, :, d], ypeer[d])
        msg(('y2g', d), gtc.at[frm, d], gtc.at[2, d], ypeer[d])
        for i in range(3):
            msg(('y3', i, d), xyo.at[i, 0, :, 0], xyo.at[i, 0, :, at], ypeer[d])
            msg(('y3g', i, d), gto.at[i, 0, 0], gto.at[i, 0, at], ypeer[d])
            msg(('y4', i, d), xyo.at[i, 0, k, frm], xyo.at[i, 0, k, 2], ypeer[d])
        for r in range(SIDE):
            msg(('x3', r, d), xyc.at[r, :, 1], xyo.at[at - 1, 1, :, r], xpeer[d])
        msg(('x3g', d), gtc.at[:, 1], gto.at[at - 1, 1], xpeer[d])
        msg(('x4', d), xyo.at[frm - 1, 1, k], xyo.at[1, 1, k], xpeer[d])
        msg(('r1', d), con.at[2, :, d], rsh.at[d], ypeer[d])
        msg(('r1g', d), cong.at[2, d], rshg.at[d], ypeer[d])
        for h in range(2):
            src = (1, 3)[d]
            msg(('r2', h, d), con.at[src, :, h], rsf.at[d, :, h], ypeer[d])
            msg(('r2g', h, d), cong.at[src, h], rsfg.at[d, h], ypeer[d])
    msg('x2g', gto.at[0, 0, 0], gto.at[1, 0, 0], xpeer[1])
    for i in range(3):
        msg(('y4g', i), gto.at[i, 0, 1], gto.at[i, 0, 2], ypeer[1])
    msg('x4g', gto.at[0, 1], gto.at[1, 1], xpeer[1])
    for m in range(3):
        msg(('m', 0, m), wins[m], (wg, wu, wd)[m].at[1], mate)
        for i in range(1, SIDE):
            msg(('m', i, m), whs[m].at[0, i], whs[m].at[1, i], mate)
        msg(('dw', m), (dwg, dwu, dwd)[m].at[1], (dwg_out, dwu_out, dwd_out)[m].at[1], mate)

    def start(*names):
        for name in names:
            msgs[name].start()

    def arrive(*names):
        for name in names:
            msgs[name].wait_recv()

    both = range(2)
    loads = [pltpu.make_async_copy(s, t, loc_sem.at[i]) for i, (s, t) in enumerate((
        (x_hbm, xyc.at[0, 0]), (dy_hbm, xyc.at[0, 1]), (gt_hbm, gtc.at[0]),
        (wg_hbm, wg.at[0]), (wu_hbm, wu.at[0]), (wd_hbm, wd.at[0])))]
    for load in loads:
        load.start()

    barrier = pltpu.get_barrier_semaphore()
    for peer in xpeer + ypeer + (mate,):
        pl.semaphore_signal(barrier, inc=1, device_id=peer, device_id_type=MESH)
    pl.semaphore_wait(barrier, 5)

    for load in loads[:3]:
        load.wait()
    start(*[(n, d) for d in both for n in ('x1', 'x1g', 'y1', 'y1g')])
    start(*[('w1', 0, d) for d in both])
    start(*[('m', 0, m) for m in range(3)])
    for ref in (dwg, dwu, dwd):
        ref[...] = jnp.zeros_like(ref)
    for load in loads[3:]:
        load.wait()

    th, d_model = xyc.shape[3], xyc.shape[4]
    tok = 2 * th
    pk = gtc.shape[2]
    groups = th // pk
    lane = lax.broadcasted_iota(jnp.int32, (pk, LANES), 1)

    def gate_column(tables, eid):
        return jnp.concatenate([
            jnp.sum(jnp.where(lane == q * experts + eid, t, 0.0), axis=1, keepdims=True)
            for t in tables for q in range(groups)], axis=0)

    def gate_pack(column, h, eid):
        base = h * groups
        return functools.reduce(lambda p, v: p + v, [
            jnp.where(lane == q * experts + eid, column[(base + q) * pk:(base + q + 1) * pk], 0.0) for q in range(groups)])

    def acts(x, gate, w):
        xm = x * jnp.where(gate > 0.0, 1.0, 0.0).astype(BF16)
        a = dot(xm, wg[w], 1, 0)
        b = dot(xm, wu[w], 1, 0)
        sig = jax.nn.sigmoid(a)
        silu = a * sig
        return a, b, sig, silu, (silu * b).astype(BF16)

    def act_grads(g, a, b, sig, silu, w):
        dh = dot(g, wd[w], 1, 1)
        return (dh * b * sig * (1.0 + a * (1.0 - sig))).astype(BF16), (dh * silu).astype(BF16)

    def weight_grads(x, h, g, da, db, e):
        dwd[e] += dot(h, g, 0, 0)
        dwg[e] += dot(x, da, 0, 0)
        dwu[e] += dot(x, db, 0, 0)

    def column_task(r, w, eid, first, grads):
        gate = gate_column([gtc[r, 0], gtc[r, 1]], eid)
        x = xyc[r, 0].reshape(tok, d_model)
        dy32 = xyc[r, 1].reshape(tok, d_model).astype(F32)
        a, b, sig, silu, h = acts(x, gate, w)
        o = dot(h, wd[w], 1, 0).astype(BF16).astype(F32)
        yc = (gate * o).reshape(2, th, d_model)
        dg = jnp.sum(dy32 * o, axis=1, keepdims=True)
        g = (gate * dy32).astype(BF16)
        da, db = act_grads(g, a, b, sig, silu, w)
        dxc = (dot(da, wg[w], 1, 1) + dot(db, wu[w], 1, 1)).astype(BF16).astype(F32).reshape(2, th, d_model)

        if first is not None:
            @pl.when(first)
            def _():
                con[r] = jnp.zeros_like(con[r])
                cong[r] = jnp.zeros_like(cong[r])
        con[r, 0] += yc
        con[r, 1] += dxc
        for h2 in range(2):
            cong[r, h2] += gate_pack(dg, h2, eid)
        if grads is not None:
            weight_grads(x, h, g, da, db, grads)

    def other_task(i, half, pair, e):
        eid = expert_id(e, 0)
        r = 2 * pair
        gate = gate_column([gto[i, half, r], gto[i, half, r + 1]], eid)
        x = xyo[i, half, 0, pl.ds(r, 2)].reshape(tok, d_model)
        dy32 = xyo[i, half, 1, pl.ds(r, 2)].reshape(tok, d_model).astype(F32)
        a, b, sig, silu, h = acts(x, gate, e)
        g = (gate * dy32).astype(BF16)
        da, db = act_grads(g, a, b, sig, silu, e)
        weight_grads(x, h, g, da, db, e)

    def at_step(t, n):
        return pl.when(t == n)

    def own_step(t, _):
        u, e = t // 2, t % 2
        r = u + u // 2 - 2 * (u // 3)

        @at_step(t, 1)
        def _():
            arrive(*[('m', 0, m) for m in range(3)])

        @at_step(t, 2)
        def _():
            arrive(*[(n, d) for d in both for n in ('x1', 'x1g')])
            start(('x2', 0), ('x2', 1), 'x2g')
            start(*[('w1', m, d) for m in (1, 2) for d in both])
            arrive(*[(n, d) for d in both for n in ('y1', 'y1g')])
            start(*[(n, d) for d in both for n in ('y2', 'y2g')])
            start(*[(n, i, d) for i in (0, 2) for d in both for n in ('y3', 'y3g')])

        @at_step(t, 6)
        def _():
            arrive(*[(n, d) for d in both for n in ('y2', 'y2g')])
            arrive(('x2', 0), ('x2', 1), 'x2g')
            start(*[(n, 1, d) for d in both for n in ('y3', 'y3g')])

        column_task(r, e, expert_id(e, 0), e == 0, e)
        return 0

    lax.fori_loop(0, 2 * SIDE, own_step, 0)

    def early_step(t, _):
        pair, i, e = t // 6, (t % 6) // 2, t % 2
        i = 2 * i - 3 * (i // 2)

        @at_step(t, 0)
        def _():
            arrive(*[(n, j, d) for j in (0, 2) for d in both for n in ('y3', 'y3g')])
            start(*[('y4', j, d) for j in (0, 2) for d in both], ('y4g', 0), ('y4g', 2))

        @at_step(t, 4)
        def _():
            arrive(*[(n, 1, d) for d in both for n in ('y3', 'y3g')])
            start(('y4', 1, 0), ('y4', 1, 1), ('y4g', 1))
            arrive(*[('w1', m, d) for m in (0, 1) for d in both])
            start(*[('w2', m, d) for m in (0, 1) for d in both])
            start(*[('m', j, m) for j in (1, 3) for m in (0, 1)])

        @at_step(t, 6)
        def _():
            arrive(('w1', 2, 0), ('w1', 2, 1))
            start(('w2', 2, 0), ('w2', 2, 1), ('m', 1, 2), ('m', 3, 2))
            start(*[('x3', r, d) for r in range(SIDE) for d in both], ('x3g', 0), ('x3g', 1))
            arrive(*[('y4', j, d) for j in (0, 2) for d in both], ('y4g', 0), ('y4g', 2))

        @at_step(t, 10)
        def _():
            arrive(('y4', 1, 0), ('y4', 1, 1), ('y4g', 1))

        other_task(i, 0, pair, e)
        return 0

    lax.fori_loop(0, 12, early_step, 0)

    def weight_load(p, i, slot):
        return [pltpu.make_async_copy(s.at[p, i], t.at[slot], wl_sem.at[slot - 2, m])
                for m, (s, t) in enumerate(((whg, wg), (whu, wu), (whd, wd)))]

    def load_start(p, i, slot):
        for c in weight_load(p, i, slot):
            c.start()

    def load_wait(p, i, slot):
        for c in weight_load(p, i, slot):
            c.wait()

    load_start(0, 1, 2)

    def near_step(t, _):
        v, r = t // SIDE, t % SIDE
        p, i = v // 2, 1 + 2 * (v % 2)
        slot = 2 + v % 2

        @pl.when(r == 0)
        def _():
            load_wait(p, i, slot)

            @at_step(v, 0)
            def _():
                load_start(0, 3, 3)

            @at_step(v, 1)
            def _():
                arrive(*[('m', 1, m) for m in range(3)])
                load_start(1, 1, 2)

            @at_step(v, 2)
            def _():
                arrive(*[('m', 3, m) for m in range(3)])
                load_start(1, 3, 3)

        column_task(r, slot, expert_id(p, i), None, None)
        return 0

    lax.fori_loop(0, 4 * SIDE, near_step, 0)

    arrive(*[('w2', m, d) for m in range(3) for d in both])
    start(*[('m', 2, m) for m in range(3)])
    load_start(0, 2, 2)
    load_wait(0, 2, 2)

    def far_step(t, _):
        u, p = t // 2, t % 2
        r = 2 - u + 3 * (u // 2) - 2 * (u // 3)

        @at_step(t, 1)
        def _():
            arrive(*[('m', 2, m) for m in range(3)])
            load_start(1, 2, 3)
            load_wait(1, 2, 3)

        @at_step(t, 2)
        def _():
            start(*[(n, d) for d in both for n in ('r1', 'r1g')])

        @at_step(t, 6)
        def _():
            start(('r2', 1, 0), ('r2g', 1, 0), ('r2', 0, 1), ('r2g', 0, 1))

        column_task(r, 2 + p, expert_id(p, 2), None, None)
        return 0

    lax.fori_loop(0, 2 * SIDE, far_step, 0)

    for d, (r, h) in enumerate(((1, 0), (3, 1))):
        arrive(('r1', d), ('r1g', d))
        con[r, :, h] += rsh[d]
        cong[r, h] += rshg[d]
    start(('r2', 0, 0), ('r2g', 0, 0), ('r2', 1, 1), ('r2g', 1, 1))

    def late_step(t, _):
        i, pair, e = t // 4, (t % 4) // 2, t % 2
        i = 2 * i - 3 * (i // 2)

        @at_step(t, 0)
        def _():
            arrive(*[('x3', r, d) for r in range(SIDE) for d in both], ('x3g', 0), ('x3g', 1))
            start(('x4', 0), ('x4', 1), 'x4g')

        @at_step(t, 8)
        def _():
            arrive(('x4', 0), ('x4', 1), 'x4g')

        other_task(i, 1, pair, e)
        return 0

    lax.fori_loop(0, 12, late_step, 0)

    start(*[('dw', m) for m in range(3)])
    stores = [pltpu.make_async_copy(s.at[0], t.at[0], loc_sem.at[i]) for i, (s, t) in enumerate(
        ((dwg, dwg_out), (dwu, dwu_out), (dwd, dwd_out)))]
    for store in stores:
        store.start()
    arrive(*[(n, h, d) for h in range(2) for d in both for n in ('r2', 'r2g')])
    for h in range(2):
        rows = pl.ds(h * th, th)
        y_out[rows, :] = (con[0, 0, h] + rsf[0, 0, h] + rsf[1, 0, h]).astype(BF16)
        dx_out[rows, :] = (con[0, 1, h] + rsf[0, 1, h] + rsf[1, 1, h]).astype(BF16)
        dgt_out[h] = cong[0, h] + rsfg[0, h] + rsfg[1, h]
    arrive(*[('dw', m) for m in range(3)])
    for c in msgs.values():
        c.wait_send()
    for store in stores:
        store.wait()


def solution(mesh):
    experts = SIDE * SIDE * CORES
    assert mesh.shape['ei'] == SIDE and mesh.shape['eo'] == SIDE * CORES
    groups = LANES // experts
    tok_spec = P(('dp', 'ei', 'eo'), None)
    weight_spec = P(('ei', 'eo'), None, None)
    grad_spec = P(('dp', 'ei', 'eo'), None, None)
    hbm = pl.BlockSpec(memory_space=pl.ANY)
    vmem = pl.BlockSpec(memory_space=pltpu.VMEM)

    def device_layer(x_loc, idx_loc, gate_loc, wg_loc, wu_loc, wd_loc, dy_loc):
        tok, _ = idx_loc.shape
        d_model = x_loc.shape[1]
        d_ff = wg_loc.shape[2]
        th = tok // 2
        pk = th // groups
        hit = idx_loc[:, :, None] == jnp.arange(experts, dtype=jnp.int32)
        gates = jnp.sum(jnp.where(hit, gate_loc[:, :, None], 0.0), axis=1)
        gates = gates.reshape(2, groups, pk, experts).transpose(0, 2, 1, 3).reshape(2, pk, LANES)
        dma = pltpu.SemaphoreType.DMA
        shape = jax.ShapeDtypeStruct
        units = (8 * SIDE * SIDE + 16 * SIDE) * 3
        outs = pl.pallas_call(
            kernel,
            out_shape=(
                shape((tok, d_model), BF16), shape((tok, d_model), BF16), shape((2, pk, LANES), F32),
                shape((2, d_model, d_ff), F32), shape((2, d_model, d_ff), F32), shape((2, d_ff, d_model), F32),
                shape((2, SIDE, d_model, d_ff), BF16), shape((2, SIDE, d_model, d_ff), BF16), shape((2, SIDE, d_ff, d_model), BF16)),
            in_specs=[hbm] * 6,
            out_specs=(vmem,) * 3 + (hbm,) * 6,
            scratch_shapes=[
                pltpu.VMEM((SIDE, 2, 2, th, d_model), BF16),
                pltpu.VMEM((SIDE - 1, 2, 2, SIDE, th, d_model), BF16),
                pltpu.VMEM((SIDE, 2, pk, LANES), F32),
                pltpu.VMEM((SIDE - 1, 2, SIDE, pk, LANES), F32),
                pltpu.VMEM((SIDE, 2, 2, th, d_model), F32),
                pltpu.VMEM((SIDE, 2, pk, LANES), F32),
                pltpu.VMEM((2, 2, th, d_model), F32),
                pltpu.VMEM((2, pk, LANES), F32),
                pltpu.VMEM((2, 2, 2, th, d_model), F32),
                pltpu.VMEM((2, 2, pk, LANES), F32),
                pltpu.VMEM((4, d_model, d_ff), BF16), pltpu.VMEM((4, d_model, d_ff), BF16), pltpu.VMEM((4, d_ff, d_model), BF16),
                pltpu.VMEM((2, d_model, d_ff), F32), pltpu.VMEM((2, d_model, d_ff), F32), pltpu.VMEM((2, d_ff, d_model), F32),
                dma((N_MSG,)), dma((N_MSG,)), dma((6,)), dma((2, 3)),
            ],
            compiler_params=pltpu.CompilerParams(collective_id=0, has_side_effects=True, vmem_limit_bytes=67000000),
            cost_estimate=pl.CostEstimate(flops=2 * units * tok * d_model * d_ff, bytes_accessed=64 * tok * d_model, transcendentals=0),
        )(x_loc.reshape(2, th, d_model), dy_loc.reshape(2, th, d_model), gates, wg_loc[0], wu_loc[0], wd_loc[0])
        y_loc, dx_loc, dgt, dwg, dwu, dwd = outs[:6]
        dgt = dgt.reshape(2, pk, groups, experts).transpose(0, 2, 1, 3).reshape(tok, experts)
        dgate_loc = jnp.sum(jnp.where(hit, dgt[:, None, :], 0.0), axis=2)
        return y_loc, dx_loc, dgate_loc, (dwg[0] + dwg[1])[None], (dwu[0] + dwu[1])[None], (dwd[0] + dwd[1])[None]

    return jax.shard_map(device_layer, mesh=mesh, in_specs=(tok_spec, tok_spec, tok_spec, weight_spec, weight_spec, weight_spec, tok_spec), out_specs=(tok_spec, tok_spec, tok_spec, grad_spec, grad_spec, grad_spec), check_vma=False)
```

```python
import functools

import jax
import jax.numpy as jnp
from jax import lax
from jax.experimental import pallas as pl
from jax.experimental.pallas import tpu as pltpu
from jax.sharding import PartitionSpec as P

MESH = pl.DeviceIdType.MESH
SIDE = 4
CORES = 2
LANES = 128
F32 = jnp.float32
BF16 = jnp.bfloat16
N_MSG = 96


def dot(a, b, dim_a, dim_b):
    return lax.dot_general(a, b, (((dim_a,), (dim_b,)), ((), ())), preferred_element_type=F32)


def kernel(x_hbm, dy_hbm, gt_hbm, wg_hbm, wu_hbm, wd_hbm,
           y_out, dx_out, dgt_out, dwg_out, dwu_out, dwd_out, whg, whu, whd,
           xyc, xyo, gtc, gto, con, cong, rsh, rshg, rsf, rsfg, wg, wu, wd, dwg, dwu, dwd,
           send_sem, recv_sem, loc_sem, wl_sem):
    dp = lax.axis_index('dp')
    row = lax.axis_index('ei')
    eo = lax.axis_index('eo')
    col, core = eo // CORES, eo % CORES
    experts = SIDE * SIDE * CORES

    def dev(c, r, k):
        return (dp, (r + SIDE) % SIDE, ((c + SIDE) % SIDE) * CORES + k)

    xpeer = (dev(col + 1, row, core), dev(col - 1, row, core))
    ypeer = (dev(col, row + 1, core), dev(col, row - 1, core))
    mate = dev(col, row, 1 - core)

    def expert_id(p, i):
        return row * SIDE * CORES + ((col + i) % SIDE) * CORES + (core + p) % CORES

    msgs = {}

    def msg(name, src, dst, peer):
        n = len(msgs)
        assert n < N_MSG
        msgs[name] = pltpu.make_async_remote_copy(
            src_ref=src, dst_ref=dst, send_sem=send_sem.at[n], recv_sem=recv_sem.at[n], device_id=peer, device_id_type=MESH)

    d_ff2, d_model2 = wd.shape[1] // 2, wg.shape[1] // 2
    wins, whs, halves = (wg_hbm, wu_hbm, wd_hbm), (whg, whu, whd), (d_model2, d_model2, d_ff2)
    for d in range(2):
        at, frm = (3, 1)[d], (3, 1)[d]
        msg(('x1', d), xyc.at[0, :, 0], xyo.at[at - 1, 0, :, 0], xpeer[d])
        msg(('x1g', d), gtc.at[0, 0], gto.at[at - 1, 0, 0], xpeer[d])
        k = 1 - d
        msg(('x2', d), xyo.at[frm - 1, 0, k, 0], xyo.at[1, 0, k, 0], xpeer[d])
        for m in range(3):
            msg(('w1', m, d), wins[m], whs[m].at[0, at], xpeer[d])
            rows = pl.ds(d * halves[m], halves[m])
            msg(('w2', m, d), whs[m].at[0, frm, rows], whs[m].at[0, 2, rows], xpeer[d])
        msg(('y1', d), xyc.at[0], xyc.at[at], ypeer[d])
        msg(('y1g', d), gtc.at[0], gtc.at[at], ypeer[d])
        msg(('y2', d), xyc.at[frm, :, d], xyc.at[2, :, d], ypeer[d])
        msg(('y2g', d), gtc.at[frm, d], gtc.at[2, d], ypeer[d])
        for i in range(3):
            msg(('y3', i, d), xyo.at[i, 0, :, 0], xyo.at[i, 0, :, at], ypeer[d])
            msg(('y3g', i, d), gto.at[i, 0, 0], gto.at[i, 0, at], ypeer[d])
            msg(('y4', i, d), xyo.at[i, 0, k, frm], xyo.at[i, 0, k, 2], ypeer[d])
        for r in range(SIDE):
            msg(('x3', r, d), xyc.at[r, :, 1], xyo.at[at - 1, 1, :, r], xpeer[d])
        msg(('x3g', d), gtc.at[:, 1], gto.at[at - 1, 1], xpeer[d])
        for p in range(2):
            rr = pl.ds(2 * p, 2)
            msg(('x4', p, d), xyo.at[frm - 1, 1, k, rr], xyo.at[1, 1, k, rr], xpeer[d])
        msg(('r1', d), con.at[2, :, d], rsh.at[d], ypeer[d])
        msg(('r1g', d), cong.at[2, d], rshg.at[d], ypeer[d])
        for h in range(2):
            src = (1, 3)[d]
            msg(('r2', h, d), con.at[src, :, h], rsf.at[d, :, h], ypeer[d])
            msg(('r2g', h, d), cong.at[src, h], rsfg.at[d, h], ypeer[d])
    msg('x2g', gto.at[0, 0, 0], gto.at[1, 0, 0], xpeer[1])
    for i in range(3):
        msg(('y4g', i), gto.at[i, 0, 1], gto.at[i, 0, 2], ypeer[1])
    msg('x4g', gto.at[0, 1], gto.at[1, 1], xpeer[1])
    for m in range(3):
        msg(('m', 0, m), wins[m], (wg, wu, wd)[m].at[1], mate)
        for i in range(1, SIDE):
            msg(('m', i, m), whs[m].at[0, i], whs[m].at[1, i], mate)
        msg(('dw', m), (dwg, dwu, dwd)[m].at[1], (dwg_out, dwu_out, dwd_out)[m].at[1], mate)

    def start(*names):
        for name in names:
            msgs[name].start()

    def arrive(*names):
        first = names[0] if isinstance(names[0], tuple) else (names[0],)
        with jax.named_scope('wait_' + '_'.join(str(v) for v in first)):
            for name in names:
                msgs[name].wait_recv()

    both = range(2)
    loads = [pltpu.make_async_copy(s, t, loc_sem.at[i]) for i, (s, t) in enumerate((
        (x_hbm, xyc.at[0, 0]), (dy_hbm, xyc.at[0, 1]), (gt_hbm, gtc.at[0]),
        (wg_hbm, wg.at[0]), (wu_hbm, wu.at[0]), (wd_hbm, wd.at[0])))]
    for load in loads:
        load.start()

    barrier = pltpu.get_barrier_semaphore()
    for peer in xpeer + ypeer + (mate,):
        pl.semaphore_signal(barrier, inc=1, device_id=peer, device_id_type=MESH)
    with jax.named_scope('wait_barrier'):
        pl.semaphore_wait(barrier, 5)

    with jax.named_scope('wait_tok'):
        for load in loads[:3]:
            load.wait()
    start(*[(n, d) for d in both for n in ('x1', 'x1g', 'y1', 'y1g')])
    start(*[('w1', 0, d) for d in both])
    start(*[('m', 0, m) for m in range(3)])
    for ref in (dwg, dwu, dwd):
        ref[...] = jnp.zeros_like(ref)
    for load in loads[3:]:
        load.wait()

    th, d_model = xyc.shape[3], xyc.shape[4]
    tok = 2 * th
    pk = gtc.shape[2]
    groups = th // pk
    lane = lax.broadcasted_iota(jnp.int32, (pk, LANES), 1)

    def gate_column(tables, eid):
        return jnp.concatenate([
            jnp.sum(jnp.where(lane == q * experts + eid, t, 0.0), axis=1, keepdims=True)
            for t in tables for q in range(groups)], axis=0)

    def gate_pack(column, h, eid):
        base = h * groups
        return functools.reduce(lambda p, v: p + v, [
            jnp.where(lane == q * experts + eid, column[(base + q) * pk:(base + q + 1) * pk], 0.0) for q in range(groups)])

    def acts(x, gate, w):
        xm = x * jnp.where(gate > 0.0, 1.0, 0.0).astype(BF16)
        a = dot(xm, wg[w], 1, 0)
        b = dot(xm, wu[w], 1, 0)
        sig = jax.nn.sigmoid(a)
        silu = a * sig
        return a, b, sig, silu, (silu * b).astype(BF16)

    def act_grads(g, a, b, sig, silu, w):
        dh = dot(g, wd[w], 1, 1)
        return (dh * b * sig * (1.0 + a * (1.0 - sig))).astype(BF16), (dh * silu).astype(BF16)

    def weight_grads(x, h, g, da, db, e):
        dwd[e] += dot(h, g, 0, 0)
        dwg[e] += dot(x, da, 0, 0)
        dwu[e] += dot(x, db, 0, 0)

    def column_task(r, w, eid, first, grads):
        gate = gate_column([gtc[r, 0], gtc[r, 1]], eid)
        x = xyc[r, 0].reshape(tok, d_model)
        dy32 = xyc[r, 1].reshape(tok, d_model).astype(F32)
        a, b, sig, silu, h = acts(x, gate, w)
        o = dot(h, wd[w], 1, 0).astype(BF16).astype(F32)
        yc = (gate * o).reshape(2, th, d_model)
        dg = jnp.sum(dy32 * o, axis=1, keepdims=True)
        g = (gate * dy32).astype(BF16)
        da, db = act_grads(g, a, b, sig, silu, w)
        dxc = (dot(da, wg[w], 1, 1) + dot(db, wu[w], 1, 1)).astype(BF16).astype(F32).reshape(2, th, d_model)

        if first is not None:
            @pl.when(first)
            def _():
                con[r] = jnp.zeros_like(con[r])
                cong[r] = jnp.zeros_like(cong[r])
        con[r, 0] += yc
        con[r, 1] += dxc
        for h2 in range(2):
            cong[r, h2] += gate_pack(dg, h2, eid)
        if grads is not None:
            weight_grads(x, h, g, da, db, grads)

    def other_task(i, half, pair, e):
        eid = expert_id(e, 0)
        r = 2 * pair
        gate = gate_column([gto[i, half, r], gto[i, half, r + 1]], eid)
        x = xyo[i, half, 0, pl.ds(r, 2)].reshape(tok, d_model)
        dy32 = xyo[i, half, 1, pl.ds(r, 2)].reshape(tok, d_model).astype(F32)
        a, b, sig, silu, h = acts(x, gate, e)
        g = (gate * dy32).astype(BF16)
        da, db = act_grads(g, a, b, sig, silu, e)
        weight_grads(x, h, g, da, db, e)

    def at_step(t, n):
        return pl.when(t == n)

    def own_step(t, _):
        u, e = t // 2, t % 2
        r = u + u // 2 - 2 * (u // 3)

        @at_step(t, 1)
        def _():
            arrive(*[('m', 0, m) for m in range(3)])

        @at_step(t, 2)
        def _():
            arrive(*[(n, d) for d in both for n in ('x1', 'x1g')])
            start(('x2', 0), ('x2', 1), 'x2g')
            start(*[('w1', m, d) for m in (1, 2) for d in both])
            arrive(*[(n, d) for d in both for n in ('y1', 'y1g')])
            start(*[(n, d) for d in both for n in ('y2', 'y2g')])
            start(*[(n, i, d) for i in (0, 2) for d in both for n in ('y3', 'y3g')])

        @at_step(t, 6)
        def _():
            arrive(*[(n, d) for d in both for n in ('y2', 'y2g')])
            arrive(('x2', 0), ('x2', 1), 'x2g')
            start(*[(n, 1, d) for d in both for n in ('y3', 'y3g')])

        with jax.named_scope('task9'):
            column_task(r, e, expert_id(e, 0), e == 0, e)
        return 0

    with jax.named_scope('loop_own'):
        lax.fori_loop(0, 2 * SIDE, own_step, 0)

    def side_of(n):
        return 2 * n - 3 * (n // 2)

    def weight_load(p, i, slot, m):
        s, t = ((whg, wg), (whu, wu), (whd, wd))[m]
        return pltpu.make_async_copy(s.at[p, i], t.at[slot], wl_sem.at[slot - 2, m])

    def load_start(p, i, slot, ms=(0, 1, 2)):
        for m in ms:
            weight_load(p, i, slot, m).start()

    def load_wait(p, i, slot):
        with jax.named_scope('wait_load'):
            for m in range(3):
                weight_load(p, i, slot, m).wait()

    def early_step(t, _):
        i, e = side_of(t // 2), t % 2

        @at_step(t, 0)
        def _():
            arrive(*[(n, j, d) for j in (0, 2) for d in both for n in ('y3', 'y3g')])
            start(*[('y4', j, d) for j in (0, 2) for d in both], ('y4g', 0), ('y4g', 2))

        @at_step(t, 4)
        def _():
            arrive(*[(n, 1, d) for d in both for n in ('y3', 'y3g')])
            start(('y4', 1, 0), ('y4', 1, 1), ('y4g', 1))
            arrive(*[('w1', m, d) for m in (0, 1) for d in both])
            start(*[('w2', m, d) for m in (0, 1) for d in both])
            start(*[('m', j, m) for j in (1, 3) for m in (0, 1)])
            load_start(0, 1, 2, (0, 1))
            load_start(0, 3, 3, (0, 1))

        with jax.named_scope('task6o'):
            other_task(i, 0, 0, e)
        return 0

    with jax.named_scope('loop_early'):
        lax.fori_loop(0, 6, early_step, 0)

    arrive(('w1', 2, 0), ('w1', 2, 1))
    start(('w2', 2, 0), ('w2', 2, 1), ('m', 1, 2), ('m', 3, 2))
    load_start(0, 1, 2, (2,))
    load_start(0, 3, 3, (2,))
    start(*[('x3', r, d) for r in range(SIDE) for d in both], ('x3g', 0), ('x3g', 1))

    def near_step(t, _):
        v, r = t // SIDE, t % SIDE
        p, i = v // 2, 1 + 2 * (v % 2)
        slot = 2 + v % 2

        @pl.when(r == 0)
        def _():
            load_wait(p, i, slot)

            @at_step(v, 1)
            def _():
                arrive(*[('m', 1, m) for m in range(3)])
                load_start(1, 1, 2)

            @at_step(v, 2)
            def _():
                arrive(*[('m', 3, m) for m in range(3)])
                load_start(1, 3, 3)

            @at_step(v, 3)
            def _():
                arrive(*[('w2', m, d) for m in (0, 1) for d in both])
                start(('m', 2, 0), ('m', 2, 1))
                load_start(0, 2, 2, (0, 1))

        with jax.named_scope('task6c'):
            column_task(r, slot, expert_id(p, i), None, None)
        return 0

    with jax.named_scope('loop_near'):
        lax.fori_loop(0, 4 * SIDE, near_step, 0)

    arrive(('w2', 2, 0), ('w2', 2, 1))
    start(('m', 2, 2))
    load_start(0, 2, 2, (2,))
    arrive(('m', 2, 0), ('m', 2, 1))
    load_start(1, 2, 3, (0, 1))
    load_wait(0, 2, 2)

    def far_step(t, _):
        u, p = t // 2, t % 2
        r = 2 - u + 3 * (u // 2) - 2 * (u // 3)

        @at_step(t, 1)
        def _():
            arrive(('m', 2, 2))
            load_start(1, 2, 3, (2,))
            load_wait(1, 2, 3)

        @at_step(t, 2)
        def _():
            start(*[(n, d) for d in both for n in ('r1', 'r1g')])

        @at_step(t, 6)
        def _():
            start(('r2', 1, 0), ('r2g', 1, 0), ('r2', 0, 1), ('r2g', 0, 1))

        with jax.named_scope('task6c'):
            column_task(r, 2 + p, expert_id(p, 2), None, None)
        return 0

    with jax.named_scope('loop_far'):
        lax.fori_loop(0, 2 * SIDE, far_step, 0)

    arrive(*[('y4', j, d) for j in range(3) for d in both], *[('y4g', j) for j in range(3)])

    def rest_step(t, _):
        other_task(side_of(t // 2), 0, 1, t % 2)
        return 0

    with jax.named_scope('loop_rest'):
        lax.fori_loop(0, 6, rest_step, 0)

    for d, (r, h) in enumerate(((1, 0), (3, 1))):
        arrive(('r1', d), ('r1g', d))
        con[r, :, h] += rsh[d]
        cong[r, h] += rshg[d]
    start(('r2', 0, 0), ('r2g', 0, 0), ('r2', 1, 1), ('r2g', 1, 1))

    def late_step(t, _):
        u = t - 8
        near_side = 1 - t // 8
        pair = near_side * (t // 4) + (1 - near_side) * (u // 2)
        i = near_side * 2 * ((t % 4) // 2) + (1 - near_side)
        e = 1 - t % 2

        @at_step(t, 0)
        def _():
            arrive(*[('x3', r, d) for r in (0, 1) for d in both], ('x3g', 0), ('x3g', 1))
            start(('x4', 0, 0), ('x4', 0, 1), 'x4g')

        @at_step(t, 4)
        def _():
            arrive(*[('x3', r, d) for r in (2, 3) for d in both])
            start(('x4', 1, 0), ('x4', 1, 1))

        @at_step(t, 8)
        def _():
            arrive(('x4', 0, 0), ('x4', 0, 1), 'x4g')

        @at_step(t, 10)
        def _():
            arrive(('x4', 1, 0), ('x4', 1, 1))

        @at_step(t, 11)
        def _():
            start(*[('dw', m) for m in range(3)])

        with jax.named_scope('task6o'):
            other_task(i, 1, pair, e)
        return 0

    with jax.named_scope('loop_late'):
        lax.fori_loop(0, 12, late_step, 0)

    stores = [pltpu.make_async_copy(s.at[0], t.at[0], loc_sem.at[i]) for i, (s, t) in enumerate(
        ((dwg, dwg_out), (dwu, dwu_out), (dwd, dwd_out)))]
    for store in stores:
        store.start()
    arrive(*[(n, h, d) for h in range(2) for d in both for n in ('r2', 'r2g')])
    for h in range(2):
        rows = pl.ds(h * th, th)
        y_out[rows, :] = (con[0, 0, h] + rsf[0, 0, h] + rsf[1, 0, h]).astype(BF16)
        dx_out[rows, :] = (con[0, 1, h] + rsf[0, 1, h] + rsf[1, 1, h]).astype(BF16)
        dgt_out[h] = cong[0, h] + rsfg[0, h] + rsfg[1, h]
    arrive(*[('dw', m) for m in range(3)])
    with jax.named_scope('wait_send_all'):
        for c in msgs.values():
            c.wait_send()
    with jax.named_scope('wait_store'):
        for store in stores:
            store.wait()


def finish(dwg_ref, dwu_ref, dwd_ref, y_ref, dx_ref, dwg_out, dwu_out, dwd_out, y_out, dx_out):
    for src, out in ((dwg_ref, dwg_out), (dwu_ref, dwu_out), (dwd_ref, dwd_out)):
        out[0] = src[0] + src[1]
    y_out[...] = y_ref[...]
    dx_out[...] = dx_ref[...]


def solution(mesh):
    experts = SIDE * SIDE * CORES
    assert mesh.shape['ei'] == SIDE and mesh.shape['eo'] == SIDE * CORES
    groups = LANES // experts
    tok_spec = P(('dp', 'ei', 'eo'), None)
    weight_spec = P(('ei', 'eo'), None, None)
    grad_spec = P(('dp', 'ei', 'eo'), None, None)
    hbm = pl.BlockSpec(memory_space=pl.ANY)
    vmem = pl.BlockSpec(memory_space=pltpu.VMEM)

    def device_layer(x_loc, idx_loc, gate_loc, wg_loc, wu_loc, wd_loc, dy_loc):
        tok, _ = idx_loc.shape
        d_model = x_loc.shape[1]
        d_ff = wg_loc.shape[2]
        th = tok // 2
        pk = th // groups
        hit = idx_loc[:, :, None] == jnp.arange(experts, dtype=jnp.int32)
        gates = jnp.sum(jnp.where(hit, gate_loc[:, :, None], 0.0), axis=1)
        gates = gates.reshape(2, groups, pk, experts).transpose(0, 2, 1, 3).reshape(2, pk, LANES)
        dma = pltpu.SemaphoreType.DMA
        shape = jax.ShapeDtypeStruct
        units = (8 * SIDE * SIDE + 16 * SIDE) * 3
        outs = pl.pallas_call(
            kernel,
            out_shape=(
                shape((tok, d_model), BF16), shape((tok, d_model), BF16), shape((2, pk, LANES), F32),
                shape((2, d_model, d_ff), F32), shape((2, d_model, d_ff), F32), shape((2, d_ff, d_model), F32),
                shape((2, SIDE, d_model, d_ff), BF16), shape((2, SIDE, d_model, d_ff), BF16), shape((2, SIDE, d_ff, d_model), BF16)),
            in_specs=[hbm] * 6,
            out_specs=(vmem,) * 3 + (hbm,) * 6,
            scratch_shapes=[
                pltpu.VMEM((SIDE, 2, 2, th, d_model), BF16),
                pltpu.VMEM((SIDE - 1, 2, 2, SIDE, th, d_model), BF16),
                pltpu.VMEM((SIDE, 2, pk, LANES), F32),
                pltpu.VMEM((SIDE - 1, 2, SIDE, pk, LANES), F32),
                pltpu.VMEM((SIDE, 2, 2, th, d_model), F32),
                pltpu.VMEM((SIDE, 2, pk, LANES), F32),
                pltpu.VMEM((2, 2, th, d_model), F32),
                pltpu.VMEM((2, pk, LANES), F32),
                pltpu.VMEM((2, 2, 2, th, d_model), F32),
                pltpu.VMEM((2, 2, pk, LANES), F32),
                pltpu.VMEM((4, d_model, d_ff), BF16), pltpu.VMEM((4, d_model, d_ff), BF16), pltpu.VMEM((4, d_ff, d_model), BF16),
                pltpu.VMEM((2, d_model, d_ff), F32), pltpu.VMEM((2, d_model, d_ff), F32), pltpu.VMEM((2, d_ff, d_model), F32),
                dma((N_MSG,)), dma((N_MSG,)), dma((6,)), dma((2, 3)),
            ],
            compiler_params=pltpu.CompilerParams(collective_id=0, has_side_effects=True, vmem_limit_bytes=67000000),
            cost_estimate=pl.CostEstimate(flops=2 * units * tok * d_model * d_ff, bytes_accessed=64 * tok * d_model, transcendentals=0),
        )(x_loc.reshape(2, th, d_model), dy_loc.reshape(2, th, d_model), gates, wg_loc[0], wu_loc[0], wd_loc[0])
        y_loc, dx_loc, dgt, dwg, dwu, dwd = outs[:6]
        cut = 8
        pair_spec = lambda rows, cols: pl.BlockSpec((2, rows // cut, cols), lambda n: (0, n, 0))
        one_spec = lambda rows, cols: pl.BlockSpec((1, rows // cut, cols), lambda n: (0, n, 0))
        row_spec = pl.BlockSpec((tok // cut, d_model), lambda n: (n, 0))
        dwg, dwu, dwd, y_loc, dx_loc = pl.pallas_call(
            finish,
            grid=(cut,),
            out_shape=(shape((1, d_model, d_ff), F32), shape((1, d_model, d_ff), F32), shape((1, d_ff, d_model), F32),
                       shape((tok, d_model), BF16), shape((tok, d_model), BF16)),
            in_specs=[pair_spec(d_model, d_ff), pair_spec(d_model, d_ff), pair_spec(d_ff, d_model), row_spec, row_spec],
            out_specs=(one_spec(d_model, d_ff), one_spec(d_model, d_ff), one_spec(d_ff, d_model), row_spec, row_spec),
            cost_estimate=pl.CostEstimate(flops=3 * d_model * d_ff, bytes_accessed=36 * d_model * d_ff, transcendentals=0),
        )(dwg, dwu, dwd, y_loc, dx_loc)
        dgt = dgt.reshape(2, pk, groups, experts).transpose(0, 2, 1, 3).reshape(tok, experts)
        dgate_loc = jnp.sum(jnp.where(hit, dgt[:, None, :], 0.0), axis=2)
        return y_loc, dx_loc, dgate_loc, dwg, dwu, dwd

    return jax.shard_map(device_layer, mesh=mesh, in_specs=(tok_spec, tok_spec, tok_spec, weight_spec, weight_spec, weight_spec, tok_spec), out_specs=(tok_spec, tok_spec, tok_spec, grad_spec, grad_spec, grad_spec), check_vma=False)
```

```python
import functools

import jax
import jax.numpy as jnp
from jax import lax
from jax.experimental import pallas as pl
from jax.experimental.pallas import tpu as pltpu
from jax.sharding import PartitionSpec as P

MESH = pl.DeviceIdType.MESH
SIDE = 4
CORES = 2
LANES = 128
F32 = jnp.float32
BF16 = jnp.bfloat16
N_MSG = 96


def dot(a, b, dim_a, dim_b):
    return lax.dot_general(a, b, (((dim_a,), (dim_b,)), ((), ())), preferred_element_type=F32)


def kernel(x_hbm, dy_hbm, gt_hbm, wg_hbm, wu_hbm, wd_hbm,
           y_out, dx_out, dgt_out, dwg_out, dwu_out, dwd_out, whg, whu, whd,
           xyc, xyo, gtc, gto, con, cong, rsh, rshg, rsf, rsfg, wg, wu, wd, dwg, dwu, dwd,
           send_sem, recv_sem, loc_sem, wl_sem, free_sem):
    dp = lax.axis_index('dp')
    row = lax.axis_index('ei')
    eo = lax.axis_index('eo')
    col, core = eo // CORES, eo % CORES
    experts = SIDE * SIDE * CORES

    def dev(c, r, k):
        return (dp, (r + SIDE) % SIDE, ((c + SIDE) % SIDE) * CORES + k)

    xpeer = (dev(col + 1, row, core), dev(col - 1, row, core))
    ypeer = (dev(col, row + 1, core), dev(col, row - 1, core))
    mate = dev(col, row, 1 - core)

    def expert_id(p, i):
        return row * SIDE * CORES + ((col + i) % SIDE) * CORES + (core + p) % CORES

    def loop(n, body):
        def run(t, carry):
            body(t)
            return carry
        lax.fori_loop(0, n, run, 0)

    def two(*key):
        return [key + (d,) for d in both]

    both, sides, mats = range(2), (1, 3), range(3)
    msgs = {}

    def msg(name, src, dst, peer):
        n = len(msgs)
        assert n < N_MSG
        msgs[name] = pltpu.make_async_remote_copy(
            src_ref=src, dst_ref=dst, send_sem=send_sem.at[n], recv_sem=recv_sem.at[n], device_id=peer, device_id_type=MESH)

    d_ff2, d_model2 = wd.shape[1] // 2, wg.shape[1] // 2
    wins, whs, halves = (wg_hbm, wu_hbm, wd_hbm), (whg, whu, whd), (d_model2, d_model2, d_ff2)
    for d in both:
        at = frm = sides[1 - d]
        msg(('x1', d), xyc.at[0, :, 0], xyo.at[at - 1, 0, :, 0], xpeer[d])
        msg(('x1g', d), gtc.at[0, 0], gto.at[at - 1, 0, 0], xpeer[d])
        k = 1 - d
        msg(('x2', d), xyo.at[frm - 1, 0, k, 0], xyo.at[1, 0, k, 0], xpeer[d])
        for m in mats:
            msg(('w1', m, d), wins[m], whs[m].at[0, at], xpeer[d])
            rows = pl.ds(d * halves[m], halves[m])
            msg(('w2', m, d), whs[m].at[0, frm, rows], whs[m].at[0, 2, rows], xpeer[d])
        msg(('y1', d), xyc.at[0], xyc.at[at], ypeer[d])
        msg(('y1g', d), gtc.at[0], gtc.at[at], ypeer[d])
        msg(('y2', d), xyc.at[frm, :, d], xyc.at[2, :, d], ypeer[d])
        msg(('y2g', d), gtc.at[frm, d], gtc.at[2, d], ypeer[d])
        for i in mats:
            msg(('y3', i, d), xyo.at[i, 0, :, 0], xyo.at[i, 0, :, at], ypeer[d])
            msg(('y3g', i, d), gto.at[i, 0, 0], gto.at[i, 0, at], ypeer[d])
            msg(('y4', i, d), xyo.at[i, 0, k, frm], xyo.at[i, 0, k, 2], ypeer[d])
        for r in range(SIDE):
            msg(('x3', r, d), xyc.at[r, :, 1], xyo.at[at - 1, 1, :, r], xpeer[d])
        msg(('x3g', d), gtc.at[:, 1], gto.at[at - 1, 1], xpeer[d])
        for p in both:
            rr = pl.ds(2 * p, 2)
            msg(('x4', p, d), xyo.at[frm - 1, 1, k, rr], xyo.at[1, 1, k, rr], xpeer[d])
        msg(('r1', d), con.at[2, :, d], rsh.at[d], ypeer[d])
        msg(('r1g', d), cong.at[2, d], rshg.at[d], ypeer[d])
        for h in both:
            src = sides[d]
            msg(('r2', h, d), con.at[src, :, h], rsf.at[d, :, h], ypeer[d])
            msg(('r2g', h, d), cong.at[src, h], rsfg.at[d, h], ypeer[d])
    msg('x2g', gto.at[0, 0, 0], gto.at[1, 0, 0], xpeer[1])
    for i in mats:
        msg(('y4g', i), gto.at[i, 0, 1], gto.at[i, 0, 2], ypeer[1])
    msg('x4g', gto.at[0, 1], gto.at[1, 1], xpeer[1])
    rr = pl.ds(2, 2)
    msg('tok', xyo.at[1, 1, :, rr], xyo.at[0, 0, :, rr], mate)
    msg('tokg', gto.at[1, 1, rr], gto.at[0, 0, rr], mate)
    for m in mats:
        msg(('m', 0, m), wins[m], (wg, wu, wd)[m].at[1], mate)
        for i in range(1, SIDE):
            msg(('m', i, m), whs[m].at[0, i], whs[m].at[1, i], mate)
        msg(('dw', m), (dwg, dwu, dwd)[m].at[1], (dwg_out, dwu_out, dwd_out)[m].at[1], mate)

    def start(*names):
        for name in names:
            msgs[name].start()

    def arrive(*names):
        for name in names:
            msgs[name].wait_recv()

    loads = [pltpu.make_async_copy(s, t, loc_sem.at[i]) for i, (s, t) in enumerate((
        (x_hbm, xyc.at[0, 0]), (dy_hbm, xyc.at[0, 1]), (gt_hbm, gtc.at[0]),
        (wg_hbm, wg.at[0]), (wu_hbm, wu.at[0]), (wd_hbm, wd.at[0])))]
    for load in loads:
        load.start()

    barrier = pltpu.get_barrier_semaphore()
    for peer in xpeer + ypeer + (mate,):
        pl.semaphore_signal(barrier, inc=1, device_id=peer, device_id_type=MESH)
    pl.semaphore_wait(barrier, 5)

    for load in loads[:3]:
        load.wait()
    start(*[(n, d) for d in both for n in ('x1', 'x1g', 'y1', 'y1g')])
    start(*two('w1', 0))
    start(*[('m', 0, m) for m in mats])
    for ref in (dwg, dwu, dwd):
        ref[...] = jnp.zeros_like(ref)
    for load in loads[3:]:
        load.wait()

    th, d_model = xyc.shape[3], xyc.shape[4]
    tok = 2 * th
    pk = gtc.shape[2]
    groups = th // pk
    lane = lax.broadcasted_iota(jnp.int32, (pk, LANES), 1)

    def gate_column(tables, eid):
        return jnp.concatenate([
            jnp.sum(jnp.where(lane == q * experts + eid, t, 0.0), axis=1, keepdims=True)
            for t in tables for q in range(groups)], axis=0)

    def gate_pack(column, h, eid):
        base = h * groups
        return functools.reduce(lambda p, v: p + v, [
            jnp.where(lane == q * experts + eid, column[(base + q) * pk:(base + q + 1) * pk], 0.0) for q in range(groups)])

    def acts(x, gate, w):
        xm = x * jnp.where(gate > 0.0, 1.0, 0.0).astype(BF16)
        a = dot(xm, wg[w], 1, 0)
        b = dot(xm, wu[w], 1, 0)
        sig = jax.nn.sigmoid(a)
        silu = a * sig
        return a, b, sig, silu, (silu * b).astype(BF16)

    def act_grads(g, a, b, sig, silu, w):
        dh = dot(g, wd[w], 1, 1)
        return (dh * b * sig * (1.0 + a * (1.0 - sig))).astype(BF16), (dh * silu).astype(BF16)

    def weight_grads(x, h, g, da, db, e):
        dwd[e] += dot(h, g, 0, 0)
        dwg[e] += dot(x, da, 0, 0)
        dwu[e] += dot(x, db, 0, 0)

    def column_task(r, w, eid, first, grads):
        gate = gate_column([gtc[r, 0], gtc[r, 1]], eid)
        x = xyc[r, 0].reshape(tok, d_model)
        dy32 = xyc[r, 1].reshape(tok, d_model).astype(F32)
        a, b, sig, silu, h = acts(x, gate, w)
        o = dot(h, wd[w], 1, 0).astype(BF16).astype(F32)
        yc = (gate * o).reshape(2, th, d_model)
        dg = jnp.sum(dy32 * o, axis=1, keepdims=True)
        g = (gate * dy32).astype(BF16)
        da, db = act_grads(g, a, b, sig, silu, w)
        dxc = (dot(da, wg[w], 1, 1) + dot(db, wu[w], 1, 1)).astype(BF16).astype(F32).reshape(2, th, d_model)

        if first is not None:
            @pl.when(first)
            def _():
                con[r] = jnp.zeros_like(con[r])
                cong[r] = jnp.zeros_like(cong[r])
        con[r, 0] += yc
        con[r, 1] += dxc
        for h2 in both:
            cong[r, h2] += gate_pack(dg, h2, eid)
        if grads is not None:
            weight_grads(x, h, g, da, db, grads)

    def other_task(i, half, pair, e):
        eid = expert_id(e, 0)
        r = 2 * pair
        gate = gate_column([gto[i, half, r], gto[i, half, r + 1]], eid)
        x = xyo[i, half, 0, pl.ds(r, 2)].reshape(tok, d_model)
        dy32 = xyo[i, half, 1, pl.ds(r, 2)].reshape(tok, d_model).astype(F32)
        a, b, sig, silu, h = acts(x, gate, e)
        g = (gate * dy32).astype(BF16)
        da, db = act_grads(g, a, b, sig, silu, e)
        weight_grads(x, h, g, da, db, e)

    def at_step(t, n):
        return pl.when(t == n)

    def own_step(t):
        u, e = t // 2, t % 2
        r = u + u // 2 - 2 * (u // 3)

        @at_step(t, 1)
        def _():
            arrive(*[('m', 0, m) for m in mats])

        @at_step(t, 2)
        def _():
            arrive(*[(n, d) for d in both for n in ('x1', 'x1g')])
            start(*two('x2'), 'x2g')
            start(*[('w1', m, d) for m in (1, 2) for d in both])
            arrive(*[(n, d) for d in both for n in ('y1', 'y1g')])
            start(*[(n, d) for d in both for n in ('y2', 'y2g')])
            start(*[(n, i, d) for i in (0, 2) for d in both for n in ('y3', 'y3g')])

        @at_step(t, 6)
        def _():
            arrive(*[(n, d) for d in both for n in ('y2', 'y2g')])
            arrive(*two('x2'), 'x2g')
            start(*[(n, 1, d) for d in both for n in ('y3', 'y3g')])

        column_task(r, e, expert_id(e, 0), e == 0, e)

    loop(2 * SIDE, own_step)

    def side_of(n):
        return 2 * n - 3 * (n // 2)

    def weight_load(p, i, slot, m):
        s, t = ((whg, wg), (whu, wu), (whd, wd))[m]
        return pltpu.make_async_copy(s.at[p, i], t.at[slot], wl_sem.at[slot - 2, m])

    def load_start(p, i, slot, ms=mats):
        for m in ms:
            weight_load(p, i, slot, m).start()

    def load_wait(p, i, slot):
        for m in mats:
            weight_load(p, i, slot, m).wait()

    def early_step(t):
        i, e = side_of(t // 2), t % 2

        @at_step(t, 0)
        def _():
            arrive(*[(n, j, d) for j in (0, 2) for d in both for n in ('y3', 'y3g')])
            start(*[('y4', j, d) for j in (0, 2) for d in both], ('y4g', 0), ('y4g', 2))

        @at_step(t, 4)
        def _():
            arrive(*[(n, 1, d) for d in both for n in ('y3', 'y3g')])
            start(*two('y4', 1), ('y4g', 1))
            arrive(*[('w1', m, d) for m in both for d in both])
            start(*[('w2', m, d) for m in both for d in both])
            start(*[('m', j, m) for j in sides for m in both])
            load_start(0, 1, 2, both)
            load_start(0, 3, 3, both)

        other_task(i, 0, 0, e)

    loop(6, early_step)

    arrive(*two('w1', 2))
    start(*two('w2', 2), *[('m', j, 2) for j in sides])
    load_start(0, 1, 2, (2,))
    load_start(0, 3, 3, (2,))
    start(*[('x3', r, d) for r in range(SIDE) for d in both], *two('x3g'))

    def near_expert(v):
        return v // 2, 1 + 2 * (v % 2), 2 + v % 2

    def near_step(t):
        v = t // 3 - t // 12
        r = (1 + t - 3 * v) % SIDE
        p, i, slot = near_expert(v)

        @pl.when(r == 1)
        def _():
            load_wait(p, i, slot)

            @at_step(v, 1)
            def _():
                arrive(*[('m', 1, m) for m in mats])
                load_start(1, 1, 2)

            @at_step(v, 2)
            def _():
                arrive(*[('m', 3, m) for m in mats])
                load_start(1, 3, 3)

            @at_step(v, 3)
            def _():
                arrive(*[('w2', m, d) for m in both for d in both])
                start(*two('m', 2))
                load_start(0, 2, 2, both)

        column_task(r, slot, expert_id(p, i), None, None)

    loop(13, near_step)

    arrive(*two('w2', 2))
    start(('m', 2, 2))
    load_start(0, 2, 2, (2,))
    arrive(*two('m', 2))
    load_start(1, 2, 3, both)
    load_wait(0, 2, 2)

    def far_step(t):
        u, p = t // 2, t % 2
        r = 2 - u + 3 * (u // 2) - 2 * (u // 3)

        @at_step(t, 1)
        def _():
            arrive(('m', 2, 2))
            load_start(1, 2, 3, (2,))
            load_wait(1, 2, 3)

        @at_step(t, 2)
        def _():
            start(*[(n, d) for d in both for n in ('r1', 'r1g')])

        @at_step(t, 6)
        def _():
            start(('r2', 1, 0), ('r2g', 1, 0), ('r2', 0, 1), ('r2g', 0, 1))

        column_task(r, 2 + p, expert_id(p, 2), None, None)

    loop(2 * SIDE, far_step)

    load_start(0, 1, 2)
    load_start(0, 3, 3)
    arrive(*[('y4', j, d) for j in mats for d in both], *[('y4g', j) for j in mats])

    def rest_step(t):
        other_task(side_of(t // 2), 0, 1, t % 2)

    loop(6, rest_step)

    for d in both:
        msgs.pop(('y4', 0, d)).wait_send()
    pl.semaphore_signal(free_sem, inc=1, device_id=mate, device_id_type=MESH)

    for d, (r, h) in enumerate(zip(sides, both)):
        arrive(('r1', d), ('r1g', d))
        con[r, :, h] += rsh[d]
        cong[r, h] += rshg[d]
    start(('r2', 0, 0), ('r2g', 0, 0), ('r2', 1, 1), ('r2g', 1, 1))

    def last_step(v):
        p, i, slot = near_expert(v)
        load_wait(p, i, slot)
        column_task(0, slot, expert_id(p, i), None, None)

        @at_step(v, 0)
        def _():
            load_start(1, 1, 2)

    loop(3, last_step)

    def late_step(t):
        far, tail, last = t // 8, t // 10, t // 11
        pair = (1 - far) * (t // 4) + far * tail
        i = (1 - far) * 2 * ((t % 4) // 2) + far * (1 - last)
        e = (1 - t % 2) * (1 - tail)

        @at_step(t, 0)
        def _():
            arrive(*[('x3', r, d) for r in (0, 1) for d in both], *two('x3g'))
            start(*two('x4', 0), 'x4g')

        @at_step(t, 4)
        def _():
            arrive(*[('x3', r, d) for r in (2, 3) for d in both])
            start(*two('x4', 1))

        @at_step(t, 8)
        def _():
            arrive(*two('x4', 0), 'x4g')

        @at_step(t, 10)
        def _():
            arrive(*two('x4', 1))
            pl.semaphore_wait(free_sem, 1)
            start('tok', 'tokg')

        @at_step(t, 11)
        def _():
            arrive('tok', 'tokg')

        @at_step(t, 9)
        def _():
            start(*[('dw', m) for m in mats])

        other_task(i, 1 - last, pair, e)

    loop(12, late_step)

    stores = [pltpu.make_async_copy(s.at[0], t.at[0], loc_sem.at[i]) for i, (s, t) in enumerate(
        ((dwg, dwg_out), (dwu, dwu_out), (dwd, dwd_out)))]
    for store in stores:
        store.start()
    arrive(*[(n, h, d) for h in both for d in both for n in ('r2', 'r2g')])
    for h in both:
        rows = pl.ds(h * th, th)
        y_out[rows, :] = (con[0, 0, h] + rsf[0, 0, h] + rsf[1, 0, h]).astype(BF16)
        dx_out[rows, :] = (con[0, 1, h] + rsf[0, 1, h] + rsf[1, 1, h]).astype(BF16)
        dgt_out[h] = cong[0, h] + rsfg[0, h] + rsfg[1, h]
    arrive(*[('dw', m) for m in mats])
    for c in msgs.values():
        c.wait_send()
    for store in stores:
        store.wait()


def finish(cut, dwg_in, dwu_in, dwd_in, y_in, dx_in, dwg_out, dwu_out, dwd_out, y_out, dx_out, bg, bu, bd, by, bx, in_sem, out_sem):
    jobs = []
    for m, (src, buf, out) in enumerate(((dwg_in, bg, dwg_out), (dwu_in, bu, dwu_out), (dwd_in, bd, dwd_out))):
        rows = buf.shape[1] // cut
        for n in range(cut):
            part = pl.ds(n * rows, rows)
            jobs.append((pltpu.make_async_copy(src.at[:, part], buf.at[:, part], in_sem.at[m, n]),
                         pltpu.make_async_copy(buf.at[0, part], out.at[0, part], out_sem.at[m, n]), buf, part))
    for m, (src, buf, out) in enumerate(((y_in, by, y_out), (dx_in, bx, dx_out))):
        jobs.append((pltpu.make_async_copy(src, buf, in_sem.at[3, m]), pltpu.make_async_copy(buf, out, out_sem.at[3, m]), None, None))
    for job in jobs:
        job[0].start()
    for read, write, buf, part in jobs:
        read.wait()
        if buf is not None:
            buf[0, part, :] += buf[1, part, :]
        write.start()
    for job in jobs:
        job[1].wait()


def solution(mesh):
    experts = SIDE * SIDE * CORES
    assert mesh.shape['ei'] == SIDE and mesh.shape['eo'] == SIDE * CORES
    groups = LANES // experts
    tok_spec = P(('dp', 'ei', 'eo'), None)
    weight_spec = P(('ei', 'eo'), None, None)
    grad_spec = P(('dp', 'ei', 'eo'), None, None)
    hbm = pl.BlockSpec(memory_space=pl.ANY)
    vmem = pl.BlockSpec(memory_space=pltpu.VMEM)

    def device_layer(x_loc, idx_loc, gate_loc, wg_loc, wu_loc, wd_loc, dy_loc):
        tok, _ = idx_loc.shape
        d_model = x_loc.shape[1]
        d_ff = wg_loc.shape[2]
        th = tok // 2
        pk = th // groups
        hit = idx_loc[:, :, None] == jnp.arange(experts, dtype=jnp.int32)
        gates = jnp.sum(jnp.where(hit, gate_loc[:, :, None], 0.0), axis=1)
        gates = gates.reshape(2, groups, pk, experts).transpose(0, 2, 1, 3).reshape(2, pk, LANES)
        dma = pltpu.SemaphoreType.DMA
        shape = jax.ShapeDtypeStruct
        units = (8 * SIDE * SIDE + 16 * SIDE) * 3
        outs = pl.pallas_call(
            kernel,
            out_shape=(
                shape((tok, d_model), BF16), shape((tok, d_model), BF16), shape((2, pk, LANES), F32),
                shape((2, d_model, d_ff), F32), shape((2, d_model, d_ff), F32), shape((2, d_ff, d_model), F32),
                shape((2, SIDE, d_model, d_ff), BF16), shape((2, SIDE, d_model, d_ff), BF16), shape((2, SIDE, d_ff, d_model), BF16)),
            in_specs=[hbm] * 6,
            out_specs=(vmem,) * 3 + (hbm,) * 6,
            scratch_shapes=[
                pltpu.VMEM((SIDE, 2, 2, th, d_model), BF16),
                pltpu.VMEM((SIDE - 1, 2, 2, SIDE, th, d_model), BF16),
                pltpu.VMEM((SIDE, 2, pk, LANES), F32),
                pltpu.VMEM((SIDE - 1, 2, SIDE, pk, LANES), F32),
                pltpu.VMEM((SIDE, 2, 2, th, d_model), F32),
                pltpu.VMEM((SIDE, 2, pk, LANES), F32),
                pltpu.VMEM((2, 2, th, d_model), F32),
                pltpu.VMEM((2, pk, LANES), F32),
                pltpu.VMEM((2, 2, 2, th, d_model), F32),
                pltpu.VMEM((2, 2, pk, LANES), F32),
                pltpu.VMEM((4, d_model, d_ff), BF16), pltpu.VMEM((4, d_model, d_ff), BF16), pltpu.VMEM((4, d_ff, d_model), BF16),
                pltpu.VMEM((2, d_model, d_ff), F32), pltpu.VMEM((2, d_model, d_ff), F32), pltpu.VMEM((2, d_ff, d_model), F32),
                dma((N_MSG,)), dma((N_MSG,)), dma((6,)), dma((2, 3)), pltpu.SemaphoreType.REGULAR,
            ],
            compiler_params=pltpu.CompilerParams(collective_id=0, has_side_effects=True, vmem_limit_bytes=67000000),
            cost_estimate=pl.CostEstimate(flops=2 * units * tok * d_model * d_ff, bytes_accessed=64 * tok * d_model, transcendentals=0),
        )(x_loc.reshape(2, th, d_model), dy_loc.reshape(2, th, d_model), gates, wg_loc[0], wu_loc[0], wd_loc[0])
        y_loc, dx_loc, dgt, dwg, dwu, dwd = outs[:6]
        cut = 4
        wide, tall, rows = (d_model, d_ff), (d_ff, d_model), (tok, d_model)
        dwg, dwu, dwd, y_loc, dx_loc = pl.pallas_call(
            functools.partial(finish, cut),
            out_shape=(shape((1,) + wide, F32), shape((1,) + wide, F32), shape((1,) + tall, F32), shape(rows, BF16), shape(rows, BF16)),
            in_specs=[hbm] * 5,
            out_specs=(hbm,) * 5,
            scratch_shapes=[pltpu.VMEM((2,) + wide, F32), pltpu.VMEM((2,) + wide, F32), pltpu.VMEM((2,) + tall, F32),
                            pltpu.VMEM(rows, BF16), pltpu.VMEM(rows, BF16), dma((4, cut)), dma((4, cut))],
            compiler_params=pltpu.CompilerParams(vmem_limit_bytes=60000000),
            cost_estimate=pl.CostEstimate(flops=3 * d_model * d_ff, bytes_accessed=36 * d_model * d_ff, transcendentals=0),
        )(dwg, dwu, dwd, y_loc, dx_loc)
        dgt = dgt.reshape(2, pk, groups, experts).transpose(0, 2, 1, 3).reshape(tok, experts)
        dgate_loc = jnp.sum(jnp.where(hit, dgt[:, None, :], 0.0), axis=2)
        return y_loc, dx_loc, dgate_loc, dwg, dwu, dwd

    return jax.shard_map(device_layer, mesh=mesh, in_specs=(tok_spec, tok_spec, tok_spec, weight_spec, weight_spec, weight_spec, tok_spec), out_specs=(tok_spec, tok_spec, tok_spec, grad_spec, grad_spec, grad_spec), check_vma=False)
```

```python
import functools

import jax
import jax.numpy as jnp
from jax import lax
from jax.experimental import pallas as pl
from jax.experimental.pallas import tpu as pltpu
from jax.sharding import PartitionSpec as P

MESH = pl.DeviceIdType.MESH
SIDE = 4
CORES = 2
LANES = 128
FAR = 4
F32 = jnp.float32
BF16 = jnp.bfloat16
N_MSG = 96


def dot(a, b, dim_a, dim_b):
    return lax.dot_general(a, b, (((dim_a,), (dim_b,)), ((), ())), preferred_element_type=F32)


def kernel(x_hbm, dy_hbm, gt_hbm, wg_hbm, wu_hbm, wd_hbm,
           y_out, dx_out, dgt_out, dwg_out, dwu_out, dwd_out, whg, whu, whd,
           xyc, xyo, gtc, gto, con, cong, rsh, rshg, rsf, rsfg, wg, wu, wd, dwg, dwu, dwd,
           send_sem, recv_sem, loc_sem, wl_sem, free_sem, slot_sem):
    dp = lax.axis_index('dp')
    row = lax.axis_index('ei')
    eo = lax.axis_index('eo')
    col, core = eo // CORES, eo % CORES
    experts = SIDE * SIDE * CORES

    def dev(c, r, k):
        return (dp, (r + SIDE) % SIDE, ((c + SIDE) % SIDE) * CORES + k)

    xpeer = (dev(col + 1, row, core), dev(col - 1, row, core))
    ypeer = (dev(col, row + 1, core), dev(col, row - 1, core))
    mate = dev(col, row, 1 - core)

    def expert_id(p, i):
        return row * SIDE * CORES + ((col + i) % SIDE) * CORES + (core + p) % CORES

    def loop(n, body):
        def run(t, carry):
            body(t)
            return carry
        lax.fori_loop(0, n, run, 0)

    def two(*key):
        return [key + (d,) for d in both]

    both, sides, mats = range(2), (1, 3), range(3)
    msgs = {}

    def msg(name, src, dst, peer):
        n = len(msgs)
        assert n < N_MSG
        msgs[name] = pltpu.make_async_remote_copy(
            src_ref=src, dst_ref=dst, send_sem=send_sem.at[n], recv_sem=recv_sem.at[n], device_id=peer, device_id_type=MESH)

    d_ff2, d_model2 = wd.shape[1] // 2, wg.shape[1] // 2
    wins, whs, halves = (wg_hbm, wu_hbm, wd_hbm), (whg, whu, whd), (d_model2, d_model2, d_ff2)
    for d in both:
        at = frm = sides[1 - d]
        msg(('x1', d), xyc.at[0, :, 0], xyo.at[at - 1, 0, :, 0], xpeer[d])
        msg(('x1g', d), gtc.at[0, 0], gto.at[at - 1, 0, 0], xpeer[d])
        k = 1 - d
        msg(('x2', d), xyo.at[frm - 1, 0, k, 0], xyo.at[1, 0, k, 0], xpeer[d])
        for m in mats:
            msg(('w1', m, d), wins[m], whs[m].at[0, at], xpeer[d])
            rows = pl.ds(d * halves[m], halves[m])
            far_dst = wd.at[FAR, rows] if m == 2 else whs[m].at[0, 2, rows]
            msg(('w2', m, d), whs[m].at[0, frm, rows], far_dst, xpeer[d])
        msg(('y1', d), xyc.at[0], xyc.at[at], ypeer[d])
        msg(('y1g', d), gtc.at[0], gtc.at[at], ypeer[d])
        msg(('y2', d), xyc.at[frm, :, d], xyc.at[2, :, d], ypeer[d])
        msg(('y2g', d), gtc.at[frm, d], gtc.at[2, d], ypeer[d])
        for i in mats:
            msg(('y3', i, d), xyo.at[i, 0, :, 0], xyo.at[i, 0, :, at], ypeer[d])
            msg(('y3g', i, d), gto.at[i, 0, 0], gto.at[i, 0, at], ypeer[d])
            msg(('y4', i, d), xyo.at[i, 0, k, frm], xyo.at[i, 0, k, 2], ypeer[d])
        for r in range(SIDE):
            msg(('x3', r, d), xyc.at[r, :, 1], xyo.at[at - 1, 1, :, r], xpeer[d])
        msg(('x3g', d), gtc.at[:, 1], gto.at[at - 1, 1], xpeer[d])
        for p in both:
            rr = pl.ds(2 * p, 2)
            msg(('x4', p, d), xyo.at[frm - 1, 1, k, rr], xyo.at[1, 1, k, rr], xpeer[d])
        msg(('r1', d), con.at[2, :, d], rsh.at[d], ypeer[d])
        msg(('r1g', d), cong.at[2, d], rshg.at[d], ypeer[d])
        for h in both:
            src = sides[d]
            msg(('r2', h, d), con.at[src, :, h], rsf.at[d, :, h], ypeer[d])
            msg(('r2g', h, d), cong.at[src, h], rsfg.at[d, h], ypeer[d])
    msg('x2g', gto.at[0, 0, 0], gto.at[1, 0, 0], xpeer[1])
    for i in mats:
        msg(('y4g', i), gto.at[i, 0, 1], gto.at[i, 0, 2], ypeer[1])
    msg('x4g', gto.at[0, 1], gto.at[1, 1], xpeer[1])
    rr = pl.ds(2, 2)
    msg('tok', xyo.at[1, 1, :, rr], xyo.at[0, 0, :, rr], mate)
    msg('tokg', gto.at[1, 1, rr], gto.at[0, 0, rr], mate)
    for m in mats:
        msg(('m', 0, m), wins[m], (wg, wu, wd)[m].at[1], mate)
        for i in range(1, SIDE):
            near = i != 2 or m != 2
            msg(('m', i, m), whs[m].at[0, i] if near else wd.at[FAR], whs[m].at[1, i] if near else wd.at[2], mate)
        msg(('dw', m), (dwg, dwu, dwd)[m].at[1], (dwg_out, dwu_out, dwd_out)[m].at[1], mate)

    def start(*names):
        for name in names:
            msgs[name].start()

    def arrive(*names):
        for name in names:
            msgs[name].wait_recv()

    loads = [pltpu.make_async_copy(s, t, loc_sem.at[i]) for i, (s, t) in enumerate((
        (x_hbm, xyc.at[0, 0]), (dy_hbm, xyc.at[0, 1]), (gt_hbm, gtc.at[0]),
        (wg_hbm, wg.at[0]), (wu_hbm, wu.at[0]), (wd_hbm, wd.at[0])))]
    for load in loads:
        load.start()

    barrier = pltpu.get_barrier_semaphore()
    for peer in xpeer + ypeer + (mate,):
        pl.semaphore_signal(barrier, inc=1, device_id=peer, device_id_type=MESH)
    pl.semaphore_wait(barrier, 5)

    for load in loads[:3]:
        load.wait()
    start(*[(n, d) for d in both for n in ('x1', 'x1g', 'y1', 'y1g')])
    start(*two('w1', 0))
    start(*[('m', 0, m) for m in mats])
    for ref in (dwg, dwu, dwd):
        ref[...] = jnp.zeros_like(ref)
    for load in loads[3:]:
        load.wait()

    th, d_model = xyc.shape[3], xyc.shape[4]
    tok = 2 * th
    pk = gtc.shape[2]
    groups = th // pk
    lane = lax.broadcasted_iota(jnp.int32, (pk, LANES), 1)

    def gate_column(tables, eid):
        return jnp.concatenate([
            jnp.sum(jnp.where(lane == q * experts + eid, t, 0.0), axis=1, keepdims=True)
            for t in tables for q in range(groups)], axis=0)

    def gate_pack(column, h, eid):
        base = h * groups
        return functools.reduce(lambda p, v: p + v, [
            jnp.where(lane == q * experts + eid, column[(base + q) * pk:(base + q + 1) * pk], 0.0) for q in range(groups)])

    def acts(x, gate, w):
        xm = x * jnp.where(gate > 0.0, 1.0, 0.0).astype(BF16)
        a = dot(xm, wg[w], 1, 0)
        b = dot(xm, wu[w], 1, 0)
        sig = jax.nn.sigmoid(a)
        silu = a * sig
        return a, b, sig, silu, (silu * b).astype(BF16)

    def act_grads(g, a, b, sig, silu, down):
        dh = dot(g, wd[down], 1, 1)
        return (dh * b * sig * (1.0 + a * (1.0 - sig))).astype(BF16), (dh * silu).astype(BF16)

    def weight_grads(x, h, g, da, db, e):
        dwd[e] += dot(h, g, 0, 0)
        dwg[e] += dot(x, da, 0, 0)
        dwu[e] += dot(x, db, 0, 0)

    def column_task(r, w, down, eid, first, grads):
        gate = gate_column([gtc[r, 0], gtc[r, 1]], eid)
        x = xyc[r, 0].reshape(tok, d_model)
        dy32 = xyc[r, 1].reshape(tok, d_model).astype(F32)
        a, b, sig, silu, h = acts(x, gate, w)
        o = dot(h, wd[down], 1, 0).astype(BF16).astype(F32)
        yc = (gate * o).reshape(2, th, d_model)
        dg = jnp.sum(dy32 * o, axis=1, keepdims=True)
        g = (gate * dy32).astype(BF16)
        da, db = act_grads(g, a, b, sig, silu, down)
        dxc = (dot(da, wg[w], 1, 1) + dot(db, wu[w], 1, 1)).astype(BF16).astype(F32).reshape(2, th, d_model)

        if first is not None:
            @pl.when(first)
            def _():
                con[r] = jnp.zeros_like(con[r])
                cong[r] = jnp.zeros_like(cong[r])
        con[r, 0] += yc
        con[r, 1] += dxc
        for h2 in both:
            cong[r, h2] += gate_pack(dg, h2, eid)
        if grads is not None:
            weight_grads(x, h, g, da, db, grads)

    def other_task(i, half, pair, e):
        eid = expert_id(e, 0)
        r = 2 * pair
        gate = gate_column([gto[i, half, r], gto[i, half, r + 1]], eid)
        x = xyo[i, half, 0, pl.ds(r, 2)].reshape(tok, d_model)
        dy32 = xyo[i, half, 1, pl.ds(r, 2)].reshape(tok, d_model).astype(F32)
        a, b, sig, silu, h = acts(x, gate, e)
        g = (gate * dy32).astype(BF16)
        da, db = act_grads(g, a, b, sig, silu, e)
        weight_grads(x, h, g, da, db, e)

    def at_step(t, n):
        return pl.when(t == n)

    def own_step(t):
        u, e = t // 2, t % 2
        r = u + u // 2 - 2 * (u // 3)

        @at_step(t, 1)
        def _():
            arrive(*[('m', 0, m) for m in mats])

        @at_step(t, 2)
        def _():
            arrive(*[(n, d) for d in both for n in ('x1', 'x1g')])
            start(*two('x2'), 'x2g')
            start(*[('w1', m, d) for m in (1, 2) for d in both])
            arrive(*[(n, d) for d in both for n in ('y1', 'y1g')])
            start(*[(n, d) for d in both for n in ('y2', 'y2g')])
            start(*[(n, i, d) for i in (0, 2) for d in both for n in ('y3', 'y3g')])

        @at_step(t, 6)
        def _():
            arrive(*[(n, d) for d in both for n in ('y2', 'y2g')])
            arrive(*two('x2'), 'x2g')
            start(*[(n, 1, d) for d in both for n in ('y3', 'y3g')])

        column_task(r, e, e, expert_id(e, 0), e == 0, e)

    loop(2 * SIDE, own_step)

    def side_of(n):
        return 2 * n - 3 * (n // 2)

    def weight_load(p, i, slot, m):
        s, t = ((whg, wg), (whu, wu), (whd, wd))[m]
        return pltpu.make_async_copy(s.at[p, i], t.at[slot], wl_sem.at[slot - 2, m])

    def load_start(p, i, slot, ms=mats):
        for m in ms:
            weight_load(p, i, slot, m).start()

    def load_wait(p, i, slot, ms=mats):
        for m in ms:
            weight_load(p, i, slot, m).wait()

    def early_step(t):
        i, e = side_of(t // 2), t % 2

        @at_step(t, 0)
        def _():
            arrive(*[(n, j, d) for j in (0, 2) for d in both for n in ('y3', 'y3g')])
            start(*[('y4', j, d) for j in (0, 2) for d in both], ('y4g', 0), ('y4g', 2))

        @at_step(t, 4)
        def _():
            arrive(*[(n, 1, d) for d in both for n in ('y3', 'y3g')])
            start(*two('y4', 1), ('y4g', 1))
            arrive(*[('w1', m, d) for m in both for d in both])
            start(*[('w2', m, d) for m in both for d in both])
            start(*[('m', j, m) for j in sides for m in both])
            load_start(0, 1, 2, both)
            load_start(0, 3, 3, both)

        other_task(i, 0, 0, e)

    loop(6, early_step)

    arrive(*two('w1', 2))
    start(*two('w2', 2), *[('m', j, 2) for j in sides])
    load_start(0, 1, 2, (2,))
    load_start(0, 3, 3, (2,))
    start(*[('x3', r, d) for r in range(SIDE) for d in both], *two('x3g'))

    def near_expert(v):
        return v // 2, 1 + 2 * (v % 2), 2 + v % 2

    def near_step(t):
        v = t // 3 - t // 12
        r = (1 + t - 3 * v) % SIDE
        p, i, slot = near_expert(v)

        @pl.when(r == 1)
        def _():
            load_wait(p, i, slot)

            @at_step(v, 1)
            def _():
                arrive(*[('m', 1, m) for m in mats])
                load_start(1, 1, 2)

            @at_step(v, 2)
            def _():
                arrive(*[('m', 3, m) for m in mats])
                load_start(1, 3, 3)

            @at_step(v, 3)
            def _():
                arrive(*[('w2', m, d) for m in both for d in both])
                start(*two('m', 2))
                load_start(0, 2, 2, both)
                pl.semaphore_signal(slot_sem, inc=1, device_id=mate, device_id_type=MESH)

        column_task(r, slot, slot, expert_id(p, i), None, None)

    loop(13, near_step)

    arrive(*two('m', 2))
    load_start(1, 2, 3, both)
    load_wait(0, 2, 2, both)
    arrive(*two('w2', 2))
    pl.semaphore_wait(slot_sem, 1)
    start(('m', 2, 2))

    def far_step(t):
        u, p = t // 2, t % 2
        r = 2 - u + 3 * (u // 2) - 2 * (u // 3)

        @at_step(t, 1)
        def _():
            load_wait(1, 2, 3, both)
            arrive(('m', 2, 2))

        @at_step(t, 2)
        def _():
            start(*[(n, d) for d in both for n in ('r1', 'r1g')])

        @at_step(t, 6)
        def _():
            start(('r2', 1, 0), ('r2g', 1, 0), ('r2', 0, 1), ('r2g', 0, 1))

        column_task(r, 2 + p, FAR - 2 * p, expert_id(p, 2), None, None)

    loop(2 * SIDE, far_step)

    load_start(0, 1, 2)
    load_start(0, 3, 3)
    arrive(*[('y4', j, d) for j in mats for d in both], *[('y4g', j) for j in mats])

    def rest_step(t):
        other_task(side_of(t // 2), 0, 1, t % 2)

    loop(6, rest_step)

    for d in both:
        msgs.pop(('y4', 0, d)).wait_send()
    pl.semaphore_signal(free_sem, inc=1, device_id=mate, device_id_type=MESH)

    for d, (r, h) in enumerate(zip(sides, both)):
        arrive(('r1', d), ('r1g', d))
        con[r, :, h] += rsh[d]
        cong[r, h] += rshg[d]
    start(('r2', 0, 0), ('r2g', 0, 0), ('r2', 1, 1), ('r2g', 1, 1))

    def last_step(v):
        p, i, slot = near_expert(v)
        load_wait(p, i, slot)
        column_task(0, slot, slot, expert_id(p, i), None, None)

        @at_step(v, 0)
        def _():
            load_start(1, 1, 2)

    loop(3, last_step)

    def late_step(t):
        far, tail, last = t // 8, t // 10, t // 11
        pair = (1 - far) * (t // 4) + far * tail
        i = (1 - far) * 2 * ((t % 4) // 2) + far * (1 - last)
        e = (1 - t % 2) * (1 - tail)

        @at_step(t, 0)
        def _():
            arrive(*[('x3', r, d) for r in (0, 1) for d in both], *two('x3g'))
            start(*two('x4', 0), 'x4g')

        @at_step(t, 4)
        def _():
            arrive(*[('x3', r, d) for r in (2, 3) for d in both])
            start(*two('x4', 1))

        @at_step(t, 8)
        def _():
            arrive(*two('x4', 0), 'x4g')

        @at_step(t, 10)
        def _():
            arrive(*two('x4', 1))
            pl.semaphore_wait(free_sem, 1)
            start('tok', 'tokg')

        @at_step(t, 11)
        def _():
            arrive('tok', 'tokg')

        @at_step(t, 9)
        def _():
            start(*[('dw', m) for m in mats])

        other_task(i, 1 - last, pair, e)

    loop(12, late_step)

    stores = [pltpu.make_async_copy(s.at[0], t.at[0], loc_sem.at[i]) for i, (s, t) in enumerate(
        ((dwg, dwg_out), (dwu, dwu_out), (dwd, dwd_out)))]
    for store in stores:
        store.start()
    msgs.pop(('m', 2, 2)).wait_send()
    for h in both:
        d = 1 - h
        arrive(('r2', h, d), ('r2g', h, d))
        con[0, :, h] += rsf[d, :, h]
        cong[0, h] += rsfg[d, h]
    for h in both:
        arrive(('r2', h, h), ('r2g', h, h))
        rows = pl.ds(h * th, th)
        for k, out in enumerate((y_out, dx_out)):
            wd[FAR, pl.ds(k * tok + h * th, th)] = (con[0, k, h] + rsf[h, k, h]).astype(BF16)
            stores.append(pltpu.make_async_copy(wd.at[FAR, pl.ds(k * tok + h * th, th)], out.at[rows], loc_sem.at[4 + 2 * k + h]))
            stores[-1].start()
        dgt_out[h] = cong[0, h] + rsfg[h, h]
    arrive(*[('dw', m) for m in mats])
    for c in msgs.values():
        c.wait_send()
    for store in stores:
        store.wait()


def finish(cut, dwg_in, dwu_in, dwd_in, y_in, dx_in, dwg_out, dwu_out, dwd_out, y_out, dx_out, bg, bu, bd, by, bx, in_sem, out_sem):
    jobs = []
    for m, (src, buf, out) in enumerate(((dwg_in, bg, dwg_out), (dwu_in, bu, dwu_out), (dwd_in, bd, dwd_out))):
        rows = buf.shape[1] // cut
        for n in range(cut):
            part = pl.ds(n * rows, rows)
            jobs.append((pltpu.make_async_copy(src.at[:, part], buf.at[:, part], in_sem.at[m, n]),
                         pltpu.make_async_copy(buf.at[0, part], out.at[0, part], out_sem.at[m, n]), buf, part))
    for m, (src, buf, out) in enumerate(((y_in, by, y_out), (dx_in, bx, dx_out))):
        jobs.append((pltpu.make_async_copy(src, buf, in_sem.at[3, m]), pltpu.make_async_copy(buf, out, out_sem.at[3, m]), None, None))
    for job in jobs:
        job[0].start()
    for read, write, buf, part in jobs:
        read.wait()
        if buf is not None:
            buf[0, part, :] += buf[1, part, :]
        write.start()
    for job in jobs:
        job[1].wait()


def solution(mesh):
    experts = SIDE * SIDE * CORES
    assert mesh.shape['ei'] == SIDE and mesh.shape['eo'] == SIDE * CORES
    groups = LANES // experts
    tok_spec = P(('dp', 'ei', 'eo'), None)
    weight_spec = P(('ei', 'eo'), None, None)
    grad_spec = P(('dp', 'ei', 'eo'), None, None)
    hbm = pl.BlockSpec(memory_space=pl.ANY)
    vmem = pl.BlockSpec(memory_space=pltpu.VMEM)

    def device_layer(x_loc, idx_loc, gate_loc, wg_loc, wu_loc, wd_loc, dy_loc):
        tok, _ = idx_loc.shape
        d_model = x_loc.shape[1]
        d_ff = wg_loc.shape[2]
        th = tok // 2
        pk = th // groups
        hit = idx_loc[:, :, None] == jnp.arange(experts, dtype=jnp.int32)
        gates = jnp.sum(jnp.where(hit, gate_loc[:, :, None], 0.0), axis=1)
        gates = gates.reshape(2, groups, pk, experts).transpose(0, 2, 1, 3).reshape(2, pk, LANES)
        dma = pltpu.SemaphoreType.DMA
        shape = jax.ShapeDtypeStruct
        units = (8 * SIDE * SIDE + 16 * SIDE) * 3
        outs = pl.pallas_call(
            kernel,
            out_shape=(
                shape((tok, d_model), BF16), shape((tok, d_model), BF16), shape((2, pk, LANES), F32),
                shape((2, d_model, d_ff), F32), shape((2, d_model, d_ff), F32), shape((2, d_ff, d_model), F32),
                shape((2, SIDE, d_model, d_ff), BF16), shape((2, SIDE, d_model, d_ff), BF16), shape((2, SIDE, d_ff, d_model), BF16)),
            in_specs=[hbm] * 6,
            out_specs=(hbm,) * 2 + (vmem,) + (hbm,) * 6,
            scratch_shapes=[
                pltpu.VMEM((SIDE, 2, 2, th, d_model), BF16),
                pltpu.VMEM((SIDE - 1, 2, 2, SIDE, th, d_model), BF16),
                pltpu.VMEM((SIDE, 2, pk, LANES), F32),
                pltpu.VMEM((SIDE - 1, 2, SIDE, pk, LANES), F32),
                pltpu.VMEM((SIDE, 2, 2, th, d_model), F32),
                pltpu.VMEM((SIDE, 2, pk, LANES), F32),
                pltpu.VMEM((2, 2, th, d_model), F32),
                pltpu.VMEM((2, pk, LANES), F32),
                pltpu.VMEM((2, 2, 2, th, d_model), F32),
                pltpu.VMEM((2, 2, pk, LANES), F32),
                pltpu.VMEM((FAR, d_model, d_ff), BF16), pltpu.VMEM((FAR, d_model, d_ff), BF16), pltpu.VMEM((FAR + 1, d_ff, d_model), BF16),
                pltpu.VMEM((2, d_model, d_ff), F32), pltpu.VMEM((2, d_model, d_ff), F32), pltpu.VMEM((2, d_ff, d_model), F32),
                dma((N_MSG,)), dma((N_MSG,)), dma((8,)), dma((2, 3)), pltpu.SemaphoreType.REGULAR, pltpu.SemaphoreType.REGULAR,
            ],
            compiler_params=pltpu.CompilerParams(collective_id=0, has_side_effects=True, vmem_limit_bytes=67000000),
            cost_estimate=pl.CostEstimate(flops=2 * units * tok * d_model * d_ff, bytes_accessed=64 * tok * d_model, transcendentals=0),
        )(x_loc.reshape(2, th, d_model), dy_loc.reshape(2, th, d_model), gates, wg_loc[0], wu_loc[0], wd_loc[0])
        y_loc, dx_loc, dgt, dwg, dwu, dwd = outs[:6]
        cut = 4
        wide, tall, rows = (d_model, d_ff), (d_ff, d_model), (tok, d_model)
        dwg, dwu, dwd, y_loc, dx_loc = pl.pallas_call(
            functools.partial(finish, cut),
            out_shape=(shape((1,) + wide, F32), shape((1,) + wide, F32), shape((1,) + tall, F32), shape(rows, BF16), shape(rows, BF16)),
            in_specs=[hbm] * 5,
            out_specs=(hbm,) * 5,
            scratch_shapes=[pltpu.VMEM((2,) + wide, F32), pltpu.VMEM((2,) + wide, F32), pltpu.VMEM((2,) + tall, F32),
                            pltpu.VMEM(rows, BF16), pltpu.VMEM(rows, BF16), dma((4, cut)), dma((4, cut))],
            compiler_params=pltpu.CompilerParams(vmem_limit_bytes=60000000),
            cost_estimate=pl.CostEstimate(flops=3 * d_model * d_ff, bytes_accessed=36 * d_model * d_ff, transcendentals=0),
        )(dwg, dwu, dwd, y_loc, dx_loc)
        dgt = dgt.reshape(2, pk, groups, experts).transpose(0, 2, 1, 3).reshape(tok, experts)
        dgate_loc = jnp.sum(jnp.where(hit, dgt[:, None, :], 0.0), axis=2)
        return y_loc, dx_loc, dgate_loc, dwg, dwu, dwd

    return jax.shard_map(device_layer, mesh=mesh, in_specs=(tok_spec, tok_spec, tok_spec, weight_spec, weight_spec, weight_spec, tok_spec), out_specs=(tok_spec, tok_spec, tok_spec, grad_spec, grad_spec, grad_spec), check_vma=False)
```
